32 devices in a mesh: pa: 8 (over z, x), gz: 4 (over y, core).
Axes of the slice: x: 2, y: 2, z: 4, core: 2. Of those that a mesh axis runs over, the one named last changes fastest.
Arguments:
- source: float32 [32, 768, 768], P('gz', 'pa'), may hold values from -24 to 24
- cell_width: float32 [32], P('gz'), may hold values from 0.5 to 2
Outputs:
- potential: float32 [32, 768, 768], P('gz', 'pa')
The draws below stay inside these ranges and needn't reach their ends.
All inputs are finite; a program needn't handle non-finite values.
Results may differ from the reference program's by a relative error of at most 0.00085.
Values sent between devices are 32-bit elements; how exact they have to be, the bound alone decides.
A program may use at most 64 MiB of HBM per device.

```python
import math
import jax
import jax.numpy as jnp
from jax import lax

NX = 768
NY = 768
NZ = 32


def laplace_field(field):
    mirrored = jnp.concatenate([field[:, :, :1], field, field[:, :, -1:]], 2)
    across = 2.0 * field - mirrored[:, :, :-2] - mirrored[:, :, 2:]
    padded_rows = jnp.pad(field, ((0, 0), (1, 1), (0, 0)))
    columns = 2.0 * field - padded_rows[:, :-2, :] - padded_rows[:, 2:, :]
    padded_depth = jnp.pad(field, ((1, 1), (0, 0), (0, 0)))
    along_depth = 2.0 * field - padded_depth[:-2] - padded_depth[2:]
    return across + columns + along_depth


def draw_source(key, part):
    rough = jnp.clip(jax.random.normal(key, (NZ, NY, NX), jnp.float32), -4.0, 4.0)
    return 0.5 * laplace_field(rough)


def shard_levels(stream_key, shape, shards, smallest, top_value):
    gain, own = 1.0, jax.random.fold_in(stream_key, 6)
    for dim, shards_of in shards:
        heights = jnp.exp(jax.random.uniform(jax.random.fold_in(own, dim), (shards_of,), jnp.float32, smallest / len(shards), top_value / len(shards)))
        gain = gain * jnp.repeat(heights, shape[dim] // shards_of).reshape([-1 if axis == dim else 1 for axis in range(len(shape))])
    return gain


def setup_inputs(seed: int = 0) -> dict:
    splits = jax.random.split(jax.random.key(seed), 3)
    return {
        "source": draw_source(jax.random.fold_in(splits[2], 71), 0),
        "cell_width": jnp.clip(jnp.exp(math.log(2.0) - 1.3862944 * jax.random.uniform(splits[1], (NZ,), jnp.float32) ** shard_levels(splits[1], (NZ,), ((0, 4),), -0.2, 0.2)), 0.5, 2.0),
    }


HIGHEST = lax.Precision.HIGHEST

def cosine_table(width):
    counter = jnp.arange(width, dtype=jnp.int32)
    phases = counter[:, None] * (2 * counter[None, :] + 1) % (4 * width)
    angles = phases.astype(jnp.float32) * (math.pi / (2 * width))
    weights = jnp.where(counter == 0, math.sqrt(1.0 / width), math.sqrt(2.0 / width)).astype(jnp.float32)
    return weights[:, None] * jnp.cos(angles)

def sine_table(width):
    counter = jnp.arange(1, width + 1, dtype=jnp.int32)
    phases = counter[:, None] * counter[None, :] % (2 * (width + 1))
    angles = phases.astype(jnp.float32) * (math.pi / (width + 1))
    return math.sqrt(2.0 / (width + 1)) * jnp.sin(angles)

def eigen_first(offset, count, width):
    wavenumber = (offset + jnp.arange(count, dtype=jnp.int32)).astype(jnp.float32)
    return 4.0 * jnp.square(jnp.sin(wavenumber * (math.pi / (2 * width))))

def eigen_second(width):
    wavenumber = jnp.arange(1, width + 1, dtype=jnp.int32).astype(jnp.float32)
    return 4.0 * jnp.square(jnp.sin(wavenumber * (math.pi / (2 * (width + 1)))))

def reference(source, cell_width):
    cos_table = cosine_table(NX)
    sin_table = sine_table(NY)
    padded = jnp.pad(cell_width, 1)
    upper_coef = 2.0 / (padded[1:-1] + padded[2:])
    lower_coef = 2.0 / (padded[:-2] + padded[1:-1])
    along_x = jnp.einsum('zyi,ki->zky', source, cos_table, precision=HIGHEST)
    spectral = jnp.einsum('zkj,lj->zkl', along_x, sin_table, precision=HIGHEST)
    eigen_sum = eigen_first(0, NX, NX)[:, None] + eigen_second(NY)[None, :]

    def eliminate(previous, entries):
        below_coef, above_coef, width_cell, forcing = entries
        diagonal = below_coef + above_coef + width_cell * eigen_sum
        divisor = diagonal + below_coef * previous[0]
        ratio_now = -above_coef / divisor
        value_now = (width_cell * forcing + below_coef * previous[1]) / divisor
        return ((ratio_now, value_now), (ratio_now, value_now))
    zero_plane = jnp.zeros((NX, NY), jnp.float32)
    _, (ratios, values) = lax.scan(eliminate, (zero_plane, zero_plane), (lower_coef, upper_coef, cell_width, spectral))

    def substitute(following, entries):
        current = entries[1] - entries[0] * following
        return (current, current)
    _, solved = lax.scan(substitute, zero_plane, (ratios, values), reverse=True)
    along_y = jnp.einsum('zkl,lj->zkj', solved, sin_table, precision=HIGHEST)
    return jnp.einsum('zky,ki->zyi', along_y, cos_table, precision=HIGHEST)
```

```python
import functools

import jax
import jax.numpy as jnp
import numpy as np
from jax import lax
from jax.experimental import pallas as pl
from jax.experimental.pallas import tpu as pltpu
from jax.sharding import PartitionSpec as P

HIGH = lax.Precision.HIGH


def summed_angles(width, coarse, fine, sine):
    f32 = lambda x: jnp.asarray(x.astype(np.float32))
    ca, sa = f32(np.cos(coarse))[:, None, :], f32(np.sin(coarse))[:, None, :]
    cb, sb = f32(np.cos(fine))[None, :, :], f32(np.sin(fine))[None, :, :]
    table = sa * cb + ca * sb if sine else ca * cb - sa * sb
    return table.reshape(width, width)


def split_steps(width):
    step = next(b for b in (32, 16, 8, 1) if width % b == 0)
    return np.arange(0, width, step, dtype=np.int64)[:, None], np.arange(step, dtype=np.int64)[:, None]


def cosine_table(width):
    odd = 2 * np.arange(width, dtype=np.int64)[None, :] + 1
    a, b = (k * odd % (4 * width) * (np.pi / (2 * width)) for k in split_steps(width))
    first = jnp.arange(width)[:, None] == 0
    weights = jnp.where(first, np.sqrt(1.0 / width), np.sqrt(2.0 / width)).astype(jnp.float32)
    return weights * summed_angles(width, a, b, False)


def sine_table(width):
    j = np.arange(1, width + 1, dtype=np.int64)[None, :]
    coarse, fine = split_steps(width)
    a, b = (l * j % (2 * (width + 1)) * (np.pi / (width + 1)) for l in (coarse, fine + 1))
    return np.float32(np.sqrt(2.0 / (width + 1))) * summed_angles(width, a, b, True)


def eigen_first(offset, count, width):
    values = 4.0 * np.sin(np.arange(width) * (np.pi / (2 * width))) ** 2
    return lax.dynamic_slice_in_dim(jnp.asarray(values, jnp.float32), offset, count)[:, None]


def eigen_second(width):
    values = 4.0 * np.sin(np.arange(1, width + 1) * (np.pi / (2 * (width + 1)))) ** 2
    return jnp.asarray(values, jnp.float32)[None, :]


def tiles(rows, width, body):
    lanes = 256 if width % 256 == 0 else width

    if rows % 8:
        for c in range(0, width, lanes):
            body(slice(0, rows), pl.ds(c, lanes))
        return

    def step(r, carry):
        row = pl.ds(pl.multiple_of(r * 8, 8), 8)
        for c in range(0, width, lanes):
            body(row, pl.ds(c, lanes))
        return carry

    lax.fori_loop(0, rows // 8, step, 0)


def ends_kernel(coef, ex, ey, spectral, ends):
    depth, rows, width = spectral.shape

    def body(row, col):
        eigen = ex[row, :] + ey[:, col]
        diag = [coef[0, z] + coef[1, z] + coef[2, z] * eigen for z in range(depth)]
        force = [coef[2, z] * spectral[z, row, col] for z in range(depth)]
        inverse = 1.0 / diag[0]
        value = force[0] * inverse
        other = 1.0 / diag[depth - 1]
        front = force[depth - 1] * other
        for z in range(1, depth):
            inverse = 1.0 / (diag[z] - (coef[0, z] * coef[1, z - 1]) * inverse)
            value = (force[z] + coef[0, z] * value) * inverse
            y = depth - 1 - z
            other = 1.0 / (diag[y] - (coef[1, y] * coef[0, y + 1]) * other)
            front = (force[y] + coef[1, y] * front) * other
        ends[0, row, col] = front
        ends[1, row, col] = value

    tiles(rows, width, body)


def reduced_kernel(coef, ex, ey, ends, sides):
    blocks = ends.shape[0] // 2
    rows, width = ends.shape[1:]
    depth = coef.shape[1] // blocks

    def body(row, col):
        eigen = ex[row, :] + ey[:, col]
        p = jnp.zeros_like(eigen)
        q = jnp.zeros_like(eigen)
        saved = []
        for b in range(blocks):
            s = b * depth
            diag = [coef[0, s + z] + coef[1, s + z] + coef[2, s + z] * eigen for z in range(depth)]
            inverse = 1.0 / diag[0]
            v1 = coef[0, s] * inverse
            other = 1.0 / diag[depth - 1]
            w0 = coef[1, s + depth - 1] * other
            for z in range(1, depth):
                inverse = 1.0 / (diag[z] - (coef[0, s + z] * coef[1, s + z - 1]) * inverse)
                v1 = v1 * (coef[0, s + z] * inverse)
                y = depth - 1 - z
                other = 1.0 / (diag[y] - (coef[1, s + y] * coef[0, s + y + 1]) * other)
                w0 = w0 * (coef[1, s + y] * other)
            w1 = coef[1, s + depth - 1] * inverse
            v0 = coef[0, s] * other
            scale = 1.0 / (1.0 - v0 * q)
            a = (ends[2 * b, row, col] + v0 * p) * scale
            c = w0 * scale
            p, q = ends[2 * b + 1, row, col] + v1 * (p + q * a), v1 * q * c + w1
            saved.append((a, c, p, q))
        head = jnp.zeros_like(eigen)
        for b in reversed(range(blocks)):
            a, c, p, q = saved[b]
            sides[2 * b + 1, row, col] = head
            if b + 1 < blocks:
                sides[2 * b + 2, row, col] = p + q * head
            head = a + c * head
        sides[0, row, col] = jnp.zeros_like(eigen)

    tiles(rows, width, body)


def final_kernel(coef, ex, ey, spectral, sides, solved):
    depth, rows, width = spectral.shape

    def body(row, col):
        eigen = ex[row, :] + ey[:, col]
        ratios, values = [], []
        for z in range(depth):
            diag = coef[0, z] + coef[1, z] + coef[2, z] * eigen
            force = coef[2, z] * spectral[z, row, col]
            if z == 0:
                force = force + coef[0, z] * sides[0, row, col]
            else:
                diag = diag - coef[0, z] * ratios[-1]
                force = force + coef[0, z] * values[-1]
            if z == depth - 1:
                force = force + coef[1, z] * sides[1, row, col]
            inverse = 1.0 / diag
            ratios.append(coef[1, z] * inverse)
            values.append(force * inverse)
        x = values[-1]
        solved[depth - 1, row, col] = x
        for z in reversed(range(depth - 1)):
            x = values[z] + ratios[z] * x
            solved[z, row, col] = x

    tiles(rows, width, body)


def solve_call(kernel, leads, lead_out, coef, ex, ey, *planes):
    rows, width = planes[0].shape[1:]
    block = next((b for b in (32, 24, 16, 8) if rows % b == 0), rows)
    spec = lambda lead: pl.BlockSpec((lead, block, width), lambda i: (0, i, 0))
    return pl.pallas_call(
        kernel,
        grid=(rows // block,),
        in_specs=[
            pl.BlockSpec(memory_space=pltpu.SMEM),
            pl.BlockSpec((block, 1), lambda i: (i, 0)),
            pl.BlockSpec((1, width), lambda i: (0, 0)),
        ]
        + [spec(lead) for lead in leads],
        out_specs=spec(lead_out),
        out_shape=jax.ShapeDtypeStruct((lead_out, rows, width), jnp.float32),
    )(coef, ex, ey, *planes)


def on_device(source, cell_width):
    depth, rows_local, width_x = source.shape
    blocks = lax.axis_size("gz")
    width_y = rows_local * lax.axis_size("pa")
    cos_table = cosine_table(width_x)
    sin_table = sine_table(width_y)
    block = lax.axis_index("gz")
    widths = lax.all_gather(cell_width, "gz", tiled=True)
    padded = jnp.pad(widths, 1)
    coef = jnp.stack(
        [2.0 / (padded[:-2] + widths), 2.0 / (widths + padded[2:]), widths]
    )
    own = lax.dynamic_slice_in_dim(coef, block * depth, depth, axis=1)
    along_x = jnp.einsum("zyi,ki->zky", source, cos_table, precision=HIGH)
    spectral = jnp.einsum(
        "zkj,lj->zkl",
        lax.all_to_all(along_x, "pa", split_axis=1, concat_axis=2, tiled=True),
        sin_table,
        precision=HIGH,
    )
    kx = spectral.shape[1]
    first = lax.axis_index("pa") * kx
    part = kx // blocks
    ex = eigen_first(first, kx, width_x)
    ex_part = eigen_first(first + block * part, part, width_x)
    ey = eigen_second(width_y)
    ends = solve_call(ends_kernel, (depth,), 2, own, ex, ey, spectral)
    ends = lax.all_to_all(ends, "gz", split_axis=1, concat_axis=0, tiled=True)
    sides = solve_call(reduced_kernel, (2 * blocks,), 2 * blocks, coef, ex_part, ey, ends)
    sides = lax.all_to_all(sides, "gz", split_axis=0, concat_axis=1, tiled=True)
    solved = solve_call(final_kernel, (depth, 2), depth, own, ex, ey, spectral, sides)
    along_y = jnp.einsum("zkl,lj->zkj", solved, sin_table, precision=HIGH)
    return jnp.einsum(
        "zky,ki->zyi",
        lax.all_to_all(along_y, "pa", split_axis=2, concat_axis=1, tiled=True),
        cos_table,
        precision=HIGH,
    )


MESH = pl.DeviceIdType.MESH
NT = (((1,), (1,)), ((), ()))
NN = (((1,), (0,)), ((), ()))


def halves(x):
    hi = x.astype(jnp.bfloat16)
    return hi, (x - hi.astype(jnp.float32)).astype(jnp.bfloat16)


def block_modes(rows, kind):
    j, l = np.arange(rows), np.arange(rows)[:, None]
    if kind == 1:
        scale = np.sqrt(np.where(l == 0, 1.0, 2.0) / rows)
        angle = np.pi * l / rows
        vectors = scale * np.cos(angle * (2 * j + 1) / 2)
    else:
        angle = (2 * l + 1) * np.pi / (2 * rows + 1)
        vectors = 2.0 / np.sqrt(2 * rows + 1) * np.sin(angle * (j + 1))
    return vectors if kind < 2 else vectors[:, ::-1], 4.0 * np.sin(angle[:, 0] / 2) ** 2


def stacked(table):
    hi = table.astype(jnp.bfloat16)
    lo = (table - np.asarray(hi, np.float64)).astype(jnp.bfloat16)
    return np.block([[hi, hi], [lo, np.zeros_like(lo)]])


def tables(width, height, parts, depth):
    k, i = np.arange(width)[:, None], np.arange(width)[None, :]
    cos = np.sqrt(np.where(k == 0, 1.0, 2.0) / width) * np.cos(np.pi * (k * (2 * i + 1) % (4 * width)) / (2 * width))
    cos_hi = cos.astype(jnp.bfloat16)
    cos_lo = (cos - np.asarray(cos_hi, np.float64)).astype(jnp.bfloat16)
    rows = height // parts
    phi, edge = [], np.zeros((3, rows, 128), np.float32)
    for kind in range(3):
        vectors, values = block_modes(rows, kind)
        phi.append(np.stack([stacked(vectors), stacked(vectors.T)]))
        edge[kind, :, 0], edge[kind, :, 1], edge[kind, :, 2] = values, vectors[:, 0], vectors[:, -1]
    lam = (4.0 * np.sin(np.arange(width) * np.pi / (2 * width)) ** 2).astype(np.float32).reshape(-1, 128)
    groups = lam.shape[0]
    targets = 2 * parts
    lam_t = np.zeros((targets, 128 // targets, 128), np.float32)
    lam_t[:, :, :groups] = lam.T.reshape(targets, 128 // targets, groups)
    lam = np.pad(lam, ((0, -groups % 8), (0, 0)))
    l = np.arange(1, height + 1)[None, :]
    cut = (np.arange(1, parts) * rows)[:, None]
    sine = lambda j: np.sqrt(2.0 / (height + 1)) * np.sin(np.pi * (l * j % (2 * (height + 1))) / (height + 1))
    modes = np.concatenate([4.0 * np.sin(np.pi * l / (2 * (height + 1))) ** 2, sine(cut) - sine(cut + 1)])
    modes = np.pad(modes, ((0, -parts % 8), (0, 0))).astype(np.float32)
    return np.stack([cos_hi, cos_lo]), np.stack(phi), edge, lam, lam_t, modes


def fused_kernel(
    size, src, width, cos, phi, edge, lam, lam_t, modes, out,
    sbuf, s16, ctab, ptab, etab, ltab, lttab, mtab, wbuf, cf, bc, xb, rx, fh, inv, vv,
    cmine, cpeer, amine, apeer, a2mine, a2peer, eb, et, rb, gt, mb, ginv, gv, st, msg, rb2, e2, uo, xo, ov,
    in_sem, out_sem, w_send, w_recv, d_send, d_recv, c_send, c_recv, a_send, a_recv, a2_send, a2_recv,
    x_send, x_recv, y_send, y_recv, u_send, u_recv,
):
    parts, slab, rows, depth, pairs, part = size
    targets = 2 * parts
    zs, wide = depth * slab, 256
    lanes = pairs * depth
    p, g = lax.axis_index("pa"), lax.axis_index("gz")
    h, c = lax.div(g, 2), lax.rem(g, 2)
    me = 2 * p + h
    kind = jnp.where(p == 0, 0, jnp.where(p == parts - 1, 2, 1))
    twin = {"gz": 2 * h + 1 - c}
    across = {"gz": 2 * (1 - h) + c}
    at = lambda t: {"pa": lax.div(t, 2), "gz": 2 * lax.rem(t, 2) + c}

    def remote(source, target, send, recv, device):
        return pltpu.make_async_remote_copy(
            src_ref=source, dst_ref=target, send_sem=send, recv_sem=recv, device_id=device, device_id_type=MESH
        )

    loads = [
        pltpu.make_async_copy(a, b, in_sem.at[n])
        for n, (a, b) in enumerate(
            [(src, sbuf), (cos, ctab), (phi.at[kind], ptab), (edge.at[kind], etab), (lam, ltab), (lam_t.at[me], lttab), (modes, mtab)]
        )
    ]
    for load in loads:
        load.start()
    for z in range(slab):
        wbuf[g, z : z + 1, :] = jnp.full((1, 128), width[z], jnp.float32)

    barrier = pltpu.get_barrier_semaphore()
    pl.semaphore_signal(barrier, inc=1, device_id=twin, device_id_type=MESH)
    pl.semaphore_signal(barrier, inc=1, device_id={"gz": 2 * (1 - h) + 1 - c}, device_id_type=MESH)
    for n in range(1, targets):
        pl.semaphore_signal(barrier, inc=1, device_id=at(lax.rem(me + n, targets)), device_id_type=MESH)
    pl.semaphore_wait(barrier, targets + 1)

    widths = lambda n, who: remote(wbuf.at[who], wbuf.at[who], w_send.at[n - 1], w_recv.at[who], {"gz": lax.rem(g + n, 4)})
    for n in range(1, 4):
        widths(n, g).start()

    loads[0].wait()
    s16[0], s16[1] = halves(sbuf[...])
    loads[1].wait()
    swap = lambda j: remote(xb.at[2 * j + 1 - c], rx.at[j], d_send.at[j], d_recv.at[j], twin)

    def along_x(j, _):
        k = pl.ds(pl.multiple_of(wide * j, wide), wide)
        dot = lambda a, b: lax.dot_general(s16[a], ctab[b, k, :], NT, preferred_element_type=jnp.float32)
        product = dot(0, 0) + dot(1, 0) + dot(0, 1)
        xb[2 * j] = product[:, :128]
        xb[2 * j + 1] = product[:, 128:]
        swap(j).start()
        return _

    lax.fori_loop(0, pairs, along_x, 0)

    for n in range(1, 4):
        widths(n, lax.rem(g + n, 4)).wait_recv()
    total = 4 * slab
    w = wbuf[...].reshape(total, 128)
    z = lax.broadcasted_iota(jnp.int32, (total, 128), 0)
    cf[0] = 2.0 / (w + jnp.where(z == 0, 0.0, pltpu.roll(w, 1, 0)))
    cf[1] = 2.0 / (w + jnp.where(z == total - 1, 0.0, pltpu.roll(w, total - 1, 0)))
    cf[2] = w
    for load in loads[2:]:
        load.wait()
    for n in range(3):
        bc[n] = jnp.broadcast_to(etab[:, n : n + 1], (rows, 128))
    for n in range(parts):
        mb[n] = jnp.broadcast_to(mtab[n : n + 1, :], (8, mtab.shape[1]))

    def cell(zz):
        zc = zz + h * (depth - 1 - 2 * zz)
        row = pl.ds(depth * h + zc, 1)
        return zc, cf[h, row, :], cf[1 - h, row, :], cf[2, row, :]

    swap_c = lambda j: remote(cmine.at[j], cpeer.at[j], c_send.at[j], c_recv.at[j], across)

    def factor(j, _):
        eigen = bc[0] + ltab[pl.ds(2 * j + c, 1), :]
        ratio = jnp.zeros((rows, 128), jnp.float32)
        for zz in range(depth):
            zc, outer, inner, w = cell(zz)
            inverse = 1.0 / ((outer + inner) + w * eigen - outer * ratio)
            inv[j, zc] = inverse
            ratio = inner * inverse
        cmine[j] = ratio
        swap_c(j).start()
        return _

    lax.fori_loop(0, pairs, factor, 0)

    def transform(which, a, b):
        hi, lo = halves(jnp.concatenate([a, b], axis=1))
        both = lax.dot_general(
            ptab[which], jnp.concatenate([hi, lo], axis=0), NN, preferred_element_type=jnp.float32
        )
        both = both[:rows] + both[rows:]
        return both[:, :128], both[:, 128:]

    swap_a = lambda j: remote(amine.at[j], apeer.at[j], a_send.at[j], a_recv.at[j], across)

    def first(j, _):
        for n in range(2):
            if n:
                swap(j).wait_recv()
            for zl in range(0, slab, 2):
                a, b = (slice(rows * y, rows * (y + 1)) for y in (zl, zl + 1))
                block = (rx.at[j] if n else xb.at[2 * j + c])
                zc = slab * ((1 - c) if n else c) + zl
                fh[j, zc], fh[j, zc + 1] = transform(0, block[a, :], block[b, :])
        value = jnp.zeros((rows, 128), jnp.float32)
        for zz in range(depth):
            zc, outer, _inner, w = cell(zz)
            value = (w * fh[j, zc] + outer * value) * inv[j, zc]
            vv[j, zc] = value
        amine[j] = value
        swap_a(j).start()
        return _

    lax.fori_loop(0, pairs, first, 0)

    ones = lax.broadcasted_iota(jnp.int32, (part, 128), 1)
    tiles = mtab.shape[1] // 128
    eigen_k = [
        jnp.broadcast_to(jnp.sum(jnp.where(ones == 2 * j + c, lttab[...], 0.0), axis=1, keepdims=True), (part, 128))
        for j in range(pairs)
    ]

    def cut_factor(z, ratio):
        row = pl.ds(z, 1)
        lower, upper, w = cf[0, row, :], cf[1, row, :], cf[2, row, :]
        after = []
        for j in range(pairs):
            for q in range(tiles):
                col = slice(128 * q, 128 * q + 128)
                inverse = 1.0 / ((lower + upper) + w * (eigen_k[j] + mb[0, :, col]) - lower * ratio[j * tiles + q])
                ginv[z, part * j : part * (j + 1), col] = inverse
                after.append(upper * inverse)
        return tuple(after)

    zero = jnp.zeros((part, 128), jnp.float32)
    lax.fori_loop(0, total, cut_factor, (zero,) * (pairs * tiles))

    def middle(j, mine, peer):
        return (mine[j] + cmine[j] * peer[j]) / (1.0 - cmine[j] * cpeer[j])

    eb[2 * lanes :, :] = jnp.zeros((128 - 2 * lanes, 128), jnp.float32)

    def first_back(j, _):
        swap_c(j).wait_recv()
        swap_a(j).wait_recv()
        x = middle(j, amine, apeer)
        for zz in reversed(range(depth)):
            zc, _outer, inner, w = cell(zz)
            if zz < depth - 1:
                x = vv[j, zc] + inner * inv[j, zc] * x
            for n in range(2):
                eb[pl.ds(lanes * n + depth * j + zc, 1), :] = jnp.sum(bc[1 + n] * x, axis=0, keepdims=True)
        return _

    lax.fori_loop(0, pairs, first_back, 0)

    et[...] = jnp.transpose(eb[...])
    piece = lambda t: pl.ds(pl.multiple_of(part * t, part), part)
    send_x = lambda n, t, who: remote(et.at[piece(t), :], rb.at[who], x_send.at[n - 1], x_recv.at[who], at(t))
    for n in range(1, targets):
        send_x(n, lax.rem(me + n, targets), me).start()
    rb[me] = et[piece(me), :]
    for n in range(1, targets):
        t = lax.rem(me + n, targets)
        send_x(n, t, t).wait_recv()
    lane = lax.broadcasted_iota(jnp.int32, (part, 128), 1)
    for i in range(parts - 1):
        for y in range(2):
            jump = pltpu.roll(rb[2 * i + y], 128 - lanes, 1) - rb[2 * i + 2 + y]
            gt[2 * i + y] = jnp.where(lane < lanes, jump, 0.0)

    def cut_forward(y, value):
        value = list(value)
        for zc in range(depth):
            z = depth * y + zc
            row = pl.ds(z, 1)
            lower, w = cf[0, row, :], cf[2, row, :]
            for j in range(pairs):
                at_lane = slice(depth * j + zc, depth * j + zc + 1)
                force = [w * jnp.broadcast_to(gt[2 * i + y, :, at_lane], (part, 128)) for i in range(parts - 1)]
                for q in range(tiles):
                    col = slice(128 * q, 128 * q + 128)
                    s = j * tiles + q
                    rhs = lower * value[s]
                    for i in range(parts - 1):
                        rhs = rhs + force[i] * mb[1 + i, :, col]
                    value[s] = rhs * ginv[z, part * j : part * (j + 1), col]
                    gv[z, part * j : part * (j + 1), col] = value[s]
        return tuple(value)

    lax.fori_loop(0, 2, cut_forward, (zero,) * (pairs * tiles))

    def cut_back(n, x):
        x = list(x)
        y = 1 - n
        sums = [zero] * (parts - 1)
        for zc in reversed(range(depth)):
            z = depth * y + zc
            upper = cf[1, pl.ds(z, 1), :]
            for j in range(pairs):
                along = [zero] * (parts - 1)
                for q in range(tiles):
                    col = slice(128 * q, 128 * q + 128)
                    s = j * tiles + q
                    r = slice(part * j, part * (j + 1))
                    x[s] = gv[z, r, col] + upper * ginv[z, r, col] * x[s]
                    for i in range(parts - 1):
                        along[i] = along[i] + mb[1 + i, :, col] * x[s]
                for i in range(parts - 1):
                    sums[i] = jnp.where(lane == depth * j + zc, jnp.sum(along[i], axis=1, keepdims=True), sums[i])
        for i in range(parts - 1):
            st[2 * i + y] = gt[2 * i + y] - sums[i]
        return tuple(x)

    lax.fori_loop(0, 2, cut_back, (zero,) * (pairs * tiles))

    for q in range(parts):
        for y in range(2):
            left = st[2 * (q - 1) + y] if q else zero
            right = pltpu.roll(st[2 * q + y], lanes, 1) if q < parts - 1 else zero
            msg[2 * q + y] = left + right
    send_y = lambda n, t, who: remote(msg.at[t], rb2.at[who], y_send.at[n - 1], y_recv.at[who], at(t))
    for n in range(1, targets):
        send_y(n, lax.rem(me + n, targets), me).start()
    rb2[me] = msg[me]
    for n in range(1, targets):
        t = lax.rem(me + n, targets)
        send_y(n, t, t).wait_recv()
    e2[...] = jnp.transpose(rb2[...].reshape(128, 128))

    swap_a2 = lambda j: remote(a2mine.at[j], a2peer.at[j], a2_send.at[j], a2_recv.at[j], across)

    def second(j, _):
        value = jnp.zeros((rows, 128), jnp.float32)
        for zz in range(depth):
            zc, outer, _inner, w = cell(zz)
            left = e2[pl.ds(depth * j + zc, 1), :]
            right = e2[pl.ds(lanes + depth * j + zc, 1), :]
            force = fh[j, zc] + bc[1] * left - bc[2] * right
            value = (w * force + outer * value) * inv[j, zc]
            vv[j, zc] = value
        a2mine[j] = value
        swap_a2(j).start()
        return _

    lax.fori_loop(0, pairs, second, 0)

    swap_u = lambda j, who: remote(uo.at[j], xo.at[2 * j + who], u_send.at[j], u_recv.at[j], twin)

    def second_back(j, _):
        swap_a2(j).wait_recv()
        x = middle(j, a2mine, a2peer)
        for zz in reversed(range(depth)):
            zc, _outer, inner, w = cell(zz)
            if zz < depth - 1:
                x = vv[j, zc] + inner * inv[j, zc] * x
            fh[j, zc] = x
        for n in range(2):
            for zl in range(0, slab, 2):
                a, b = (slice(rows * y, rows * (y + 1)) for y in (zl, zl + 1))
                zc = slab * (c if n else (1 - c)) + zl
                block = xo.at[2 * j + c] if n else uo.at[j]
                block[a, :], block[b, :] = transform(1, fh[j, zc], fh[j, zc + 1])
            if n == 0:
                swap_u(j, c).start()
        return _

    lax.fori_loop(0, pairs, second_back, 0)

    def split(j, who):
        k = 2 * j + who
        cols = pl.ds(pl.multiple_of(128 * k, 128), 128)
        s16[0, :, cols], s16[1, :, cols] = halves(xo[k])

    for j in range(pairs):
        split(j, c)
    for j in range(pairs):
        swap_u(j, 1 - c).wait_recv()
        split(j, 1 - c)

    put = lambda j: pltpu.make_async_copy(
        ov.at[j], out.at[:, pl.ds(pl.multiple_of(wide * j, wide), wide)], out_sem.at[j]
    )

    def back_x(j, _):
        i = pl.ds(pl.multiple_of(wide * j, wide), wide)
        dot = lambda a, b: lax.dot_general(s16[a], ctab[b, :, i], NN, preferred_element_type=jnp.float32)
        ov[j] = dot(0, 0) + dot(1, 0) + dot(0, 1)
        put(j).start()
        return _

    lax.fori_loop(0, pairs, back_x, 0)

    for n in range(1, 4):
        widths(n, g).wait_send()
    for n in range(1, targets):
        send_x(n, lax.rem(me + n, targets), me).wait_send()
        send_y(n, lax.rem(me + n, targets), me).wait_send()
    for j in range(pairs):
        swap(j).wait_send()
        swap_c(j).wait_send()
        swap_a(j).wait_send()
        swap_a2(j).wait_send()
        swap_u(j, c).wait_send()
        put(j).wait()


def fused(source, cell_width):
    slab, rows, nx = source.shape
    parts = lax.axis_size("pa")
    pairs, depth, targets = nx // 256, 2 * slab, 2 * parts
    part = 128 // targets
    ny = rows * parts
    consts = tables(nx, ny, parts, depth)
    f32, b16, V = jnp.float32, jnp.bfloat16, pltpu.VMEM
    tall = slab * rows
    lines = (pairs, depth, rows, 128)
    plane = (pairs, rows, 128)
    cuts = (2 * slab * 2, part * pairs, ny)
    sem = lambda n: pltpu.SemaphoreType.DMA((n,))
    scratch = [
        V((tall, nx), f32), V((2, tall, nx), b16), V((2, nx, nx), b16), V((2, 2 * rows, 2 * rows), b16), V((rows, 128), f32),
        V(consts[3].shape, f32), V((part, 128), f32), V(consts[5].shape, f32), V((4, slab, 128), f32),
        V((3, 4 * slab, 128), f32), V((3, rows, 128), f32),
        V((2 * pairs, tall, 128), f32), V((pairs, tall, 128), f32), V(lines, f32), V(lines, f32), V(lines, f32),
        V(plane, f32), V(plane, f32), V(plane, f32), V(plane, f32), V(plane, f32), V(plane, f32),
        V((128, 128), f32), V((128, 128), f32), V((targets, part, 128), f32), V((targets, part, 128), f32),
        V((parts, 8, ny), f32), V(cuts, f32), V(cuts, f32),
        V((targets, part, 128), f32), V((targets, part, 128), f32), V((targets, part, 128), f32), V((128, 128), f32),
        V((pairs, tall, 128), f32), V((2 * pairs, tall, 128), f32), V((pairs, tall, 256), f32),
        sem(7), sem(pairs), sem(3), sem(4), sem(pairs), sem(pairs), sem(pairs), sem(pairs), sem(pairs), sem(pairs),
        sem(pairs), sem(pairs), sem(targets), sem(targets), sem(targets), sem(targets), sem(pairs), sem(pairs),
    ]
    hbm = pl.BlockSpec(memory_space=pltpu.HBM)
    out = pl.pallas_call(
        functools.partial(fused_kernel, (parts, slab, rows, depth, pairs, part)),
        out_shape=jax.ShapeDtypeStruct((tall, nx), f32),
        in_specs=[hbm, pl.BlockSpec(memory_space=pltpu.SMEM)] + [hbm] * 6,
        out_specs=hbm,
        scratch_shapes=scratch,
        compiler_params=pltpu.CompilerParams(
            collective_id=0, has_side_effects=True, vmem_limit_bytes=60 * 1024 * 1024
        ),
    )(source.reshape(tall, nx), cell_width, *(jnp.asarray(t) for t in consts))
    return out.reshape(slab, rows, nx)


def fits(source, parts, blocks):
    slab, rows, nx = source.shape
    return (
        blocks == 4 and parts == 8 and nx % 256 == 0 and slab == 8 and rows % 16 == 0
        and (rows * parts) % 128 == 0 and 2 * (nx // 256) * 2 * slab <= 128
    )


def per_device(source, cell_width):
    if fits(source, lax.axis_size("pa"), lax.axis_size("gz")):
        return fused(source, cell_width)
    return on_device(source, cell_width)


def solution(mesh):
    in_specs = (P("gz", "pa", None), P("gz"))
    out_specs = P("gz", "pa", None)
    return jax.shard_map(
        per_device, mesh=mesh, in_specs=in_specs, out_specs=out_specs, check_vma=False
    )
```

```python
import functools

import jax
import jax.numpy as jnp
import numpy as np
from jax import lax
from jax.experimental import pallas as pl
from jax.experimental.pallas import tpu as pltpu
from jax.sharding import PartitionSpec as P

HIGH = lax.Precision.HIGH


def summed_angles(width, coarse, fine, sine):
    f32 = lambda x: jnp.asarray(x.astype(np.float32))
    ca, sa = f32(np.cos(coarse))[:, None, :], f32(np.sin(coarse))[:, None, :]
    cb, sb = f32(np.cos(fine))[None, :, :], f32(np.sin(fine))[None, :, :]
    table = sa * cb + ca * sb if sine else ca * cb - sa * sb
    return table.reshape(width, width)


def split_steps(width):
    step = next(b for b in (32, 16, 8, 1) if width % b == 0)
    return np.arange(0, width, step, dtype=np.int64)[:, None], np.arange(step, dtype=np.int64)[:, None]


def cosine_table(width):
    odd = 2 * np.arange(width, dtype=np.int64)[None, :] + 1
    a, b = (k * odd % (4 * width) * (np.pi / (2 * width)) for k in split_steps(width))
    first = jnp.arange(width)[:, None] == 0
    weights = jnp.where(first, np.sqrt(1.0 / width), np.sqrt(2.0 / width)).astype(jnp.float32)
    return weights * summed_angles(width, a, b, False)


def sine_table(width):
    j = np.arange(1, width + 1, dtype=np.int64)[None, :]
    coarse, fine = split_steps(width)
    a, b = (l * j % (2 * (width + 1)) * (np.pi / (width + 1)) for l in (coarse, fine + 1))
    return np.float32(np.sqrt(2.0 / (width + 1))) * summed_angles(width, a, b, True)


def eigen_first(offset, count, width):
    values = 4.0 * np.sin(np.arange(width) * (np.pi / (2 * width))) ** 2
    return lax.dynamic_slice_in_dim(jnp.asarray(values, jnp.float32), offset, count)[:, None]


def eigen_second(width):
    values = 4.0 * np.sin(np.arange(1, width + 1) * (np.pi / (2 * (width + 1)))) ** 2
    return jnp.asarray(values, jnp.float32)[None, :]


def tiles(rows, width, body):
    lanes = 256 if width % 256 == 0 else width

    if rows % 8:
        for c in range(0, width, lanes):
            body(slice(0, rows), pl.ds(c, lanes))
        return

    def step(r, carry):
        row = pl.ds(pl.multiple_of(r * 8, 8), 8)
        for c in range(0, width, lanes):
            body(row, pl.ds(c, lanes))
        return carry

    lax.fori_loop(0, rows // 8, step, 0)


def ends_kernel(coef, ex, ey, spectral, ends):
    depth, rows, width = spectral.shape

    def body(row, col):
        eigen = ex[row, :] + ey[:, col]
        diag = [coef[0, z] + coef[1, z] + coef[2, z] * eigen for z in range(depth)]
        force = [coef[2, z] * spectral[z, row, col] for z in range(depth)]
        inverse = 1.0 / diag[0]
        value = force[0] * inverse
        other = 1.0 / diag[depth - 1]
        front = force[depth - 1] * other
        for z in range(1, depth):
            inverse = 1.0 / (diag[z] - (coef[0, z] * coef[1, z - 1]) * inverse)
            value = (force[z] + coef[0, z] * value) * inverse
            y = depth - 1 - z
            other = 1.0 / (diag[y] - (coef[1, y] * coef[0, y + 1]) * other)
            front = (force[y] + coef[1, y] * front) * other
        ends[0, row, col] = front
        ends[1, row, col] = value

    tiles(rows, width, body)


def reduced_kernel(coef, ex, ey, ends, sides):
    blocks = ends.shape[0] // 2
    rows, width = ends.shape[1:]
    depth = coef.shape[1] // blocks

    def body(row, col):
        eigen = ex[row, :] + ey[:, col]
        p = jnp.zeros_like(eigen)
        q = jnp.zeros_like(eigen)
        saved = []
        for b in range(blocks):
            s = b * depth
            diag = [coef[0, s + z] + coef[1, s + z] + coef[2, s + z] * eigen for z in range(depth)]
            inverse = 1.0 / diag[0]
            v1 = coef[0, s] * inverse
            other = 1.0 / diag[depth - 1]
            w0 = coef[1, s + depth - 1] * other
            for z in range(1, depth):
                inverse = 1.0 / (diag[z] - (coef[0, s + z] * coef[1, s + z - 1]) * inverse)
                v1 = v1 * (coef[0, s + z] * inverse)
                y = depth - 1 - z
                other = 1.0 / (diag[y] - (coef[1, s + y] * coef[0, s + y + 1]) * other)
                w0 = w0 * (coef[1, s + y] * other)
            w1 = coef[1, s + depth - 1] * inverse
            v0 = coef[0, s] * other
            scale = 1.0 / (1.0 - v0 * q)
            a = (ends[2 * b, row, col] + v0 * p) * scale
            c = w0 * scale
            p, q = ends[2 * b + 1, row, col] + v1 * (p + q * a), v1 * q * c + w1
            saved.append((a, c, p, q))
        head = jnp.zeros_like(eigen)
        for b in reversed(range(blocks)):
            a, c, p, q = saved[b]
            sides[2 * b + 1, row, col] = head
            if b + 1 < blocks:
                sides[2 * b + 2, row, col] = p + q * head
            head = a + c * head
        sides[0, row, col] = jnp.zeros_like(eigen)

    tiles(rows, width, body)


def final_kernel(coef, ex, ey, spectral, sides, solved):
    depth, rows, width = spectral.shape

    def body(row, col):
        eigen = ex[row, :] + ey[:, col]
        ratios, values = [], []
        for z in range(depth):
            diag = coef[0, z] + coef[1, z] + coef[2, z] * eigen
            force = coef[2, z] * spectral[z, row, col]
            if z == 0:
                force = force + coef[0, z] * sides[0, row, col]
            else:
                diag = diag - coef[0, z] * ratios[-1]
                force = force + coef[0, z] * values[-1]
            if z == depth - 1:
                force = force + coef[1, z] * sides[1, row, col]
            inverse = 1.0 / diag
            ratios.append(coef[1, z] * inverse)
            values.append(force * inverse)
        x = values[-1]
        solved[depth - 1, row, col] = x
        for z in reversed(range(depth - 1)):
            x = values[z] + ratios[z] * x
            solved[z, row, col] = x

    tiles(rows, width, body)


def solve_call(kernel, leads, lead_out, coef, ex, ey, *planes):
    rows, width = planes[0].shape[1:]
    block = next((b for b in (32, 24, 16, 8) if rows % b == 0), rows)
    spec = lambda lead: pl.BlockSpec((lead, block, width), lambda i: (0, i, 0))
    return pl.pallas_call(
        kernel,
        grid=(rows // block,),
        in_specs=[
            pl.BlockSpec(memory_space=pltpu.SMEM),
            pl.BlockSpec((block, 1), lambda i: (i, 0)),
            pl.BlockSpec((1, width), lambda i: (0, 0)),
        ]
        + [spec(lead) for lead in leads],
        out_specs=spec(lead_out),
        out_shape=jax.ShapeDtypeStruct((lead_out, rows, width), jnp.float32),
    )(coef, ex, ey, *planes)


def on_device(source, cell_width):
    depth, rows_local, width_x = source.shape
    blocks = lax.axis_size("gz")
    width_y = rows_local * lax.axis_size("pa")
    cos_table = cosine_table(width_x)
    sin_table = sine_table(width_y)
    block = lax.axis_index("gz")
    widths = lax.all_gather(cell_width, "gz", tiled=True)
    padded = jnp.pad(widths, 1)
    coef = jnp.stack(
        [2.0 / (padded[:-2] + widths), 2.0 / (widths + padded[2:]), widths]
    )
    own = lax.dynamic_slice_in_dim(coef, block * depth, depth, axis=1)
    along_x = jnp.einsum("zyi,ki->zky", source, cos_table, precision=HIGH)
    spectral = jnp.einsum(
        "zkj,lj->zkl",
        lax.all_to_all(along_x, "pa", split_axis=1, concat_axis=2, tiled=True),
        sin_table,
        precision=HIGH,
    )
    kx = spectral.shape[1]
    first = lax.axis_index("pa") * kx
    part = kx // blocks
    ex = eigen_first(first, kx, width_x)
    ex_part = eigen_first(first + block * part, part, width_x)
    ey = eigen_second(width_y)
    ends = solve_call(ends_kernel, (depth,), 2, own, ex, ey, spectral)
    ends = lax.all_to_all(ends, "gz", split_axis=1, concat_axis=0, tiled=True)
    sides = solve_call(reduced_kernel, (2 * blocks,), 2 * blocks, coef, ex_part, ey, ends)
    sides = lax.all_to_all(sides, "gz", split_axis=0, concat_axis=1, tiled=True)
    solved = solve_call(final_kernel, (depth, 2), depth, own, ex, ey, spectral, sides)
    along_y = jnp.einsum("zkl,lj->zkj", solved, sin_table, precision=HIGH)
    return jnp.einsum(
        "zky,ki->zyi",
        lax.all_to_all(along_y, "pa", split_axis=2, concat_axis=1, tiled=True),
        cos_table,
        precision=HIGH,
    )


MESH = pl.DeviceIdType.MESH
NT = (((1,), (1,)), ((), ()))
NN = (((1,), (0,)), ((), ()))
SOURCE_PIECES = 4


def halves(x):
    hi = x.astype(jnp.bfloat16)
    return hi, (x - hi.astype(jnp.float32)).astype(jnp.bfloat16)


def block_modes(rows, kind):
    j, l = np.arange(rows), np.arange(rows)[:, None]
    if kind == 1:
        scale = np.sqrt(np.where(l == 0, 1.0, 2.0) / rows)
        angle = np.pi * l / rows
        vectors = scale * np.cos(angle * (2 * j + 1) / 2)
    else:
        angle = (2 * l + 1) * np.pi / (2 * rows + 1)
        vectors = 2.0 / np.sqrt(2 * rows + 1) * np.sin(angle * (j + 1))
    return vectors if kind < 2 else vectors[:, ::-1], 4.0 * np.sin(angle[:, 0] / 2) ** 2


def stacked(table):
    hi = table.astype(jnp.bfloat16)
    lo = (table - np.asarray(hi, np.float64)).astype(jnp.bfloat16)
    return np.block([[hi, hi], [lo, np.zeros_like(lo)]])


def tables(width, height, parts, depth):
    k, i = np.arange(width)[:, None], np.arange(width)[None, :]
    cos = np.sqrt(np.where(k == 0, 1.0, 2.0) / width) * np.cos(np.pi * (k * (2 * i + 1) % (4 * width)) / (2 * width))
    cos_hi = cos.astype(jnp.bfloat16)
    cos_lo = (cos - np.asarray(cos_hi, np.float64)).astype(jnp.bfloat16)
    rows = height // parts
    phi, edge = [], np.zeros((3, rows, 128), np.float32)
    for kind in range(3):
        vectors, values = block_modes(rows, kind)
        phi.append(np.stack([stacked(vectors), stacked(vectors.T)]))
        edge[kind, :, 0], edge[kind, :, 1], edge[kind, :, 2] = values, vectors[:, 0], vectors[:, -1]
    lam = (4.0 * np.sin(np.arange(width) * np.pi / (2 * width)) ** 2).astype(np.float32).reshape(-1, 128)
    groups = lam.shape[0]
    targets = 2 * parts
    lam_t = np.zeros((targets, 128 // targets, 128), np.float32)
    lam_t[:, :, :groups] = lam.T.reshape(targets, 128 // targets, groups)
    lam = np.pad(lam, ((0, -groups % 8), (0, 0)))
    l = np.arange(1, height + 1)
    l = np.concatenate([l[::2], l[1::2]])[None, :]
    cut = (np.arange(1, parts // 2 + 1) * rows)[:, None]
    sine = lambda j: np.sqrt(2.0 / (height + 1)) * np.sin(np.pi * (l * j % (2 * (height + 1))) / (height + 1))
    modes = np.concatenate([4.0 * np.sin(np.pi * l / (2 * (height + 1))) ** 2, sine(cut) - sine(cut + 1)])
    modes = np.pad(modes, ((0, -len(modes) % 8), (0, 0))).astype(np.float32)
    return np.stack([cos_hi, cos_lo]), np.stack(phi), edge, lam, lam_t, modes


def fused_kernel(
    size, src, width, cos, phi, edge, lam, lam_t, modes, out,
    sbuf, s16, ctab, ptab, etab, ltab, lttab, mtab, wbuf, cf, bc, xb, rx, fh, inv, vv,
    inv2, cmine, cpeer, join, amine, apeer, eb, et, rb, gt, mb, ginv, gv, msg, rb2, e2, uo, xo,
    in_sem, src_sem, cos_sem, w_send, w_recv, d_send, d_recv, a_send, a_recv,
    x_send, x_recv, y_send, y_recv, u_send, u_recv,
):
    parts, slab, rows, depth, pairs, part = size
    targets = 2 * parts
    wide, lanes = 256, 4 * depth
    tall = slab * rows
    cuts, half = parts - 1, (parts - 1) // 2
    p, g = lax.axis_index("pa"), lax.axis_index("gz")
    h, c = lax.div(g, 2), lax.rem(g, 2)
    me = 2 * p + h
    kind = jnp.where(p == 0, 0, jnp.where(p == parts - 1, 2, 1))
    twin = {"gz": 2 * h + 1 - c}
    across = {"gz": 2 * (1 - h) + c}
    at = lambda t: {"pa": lax.div(t, 2), "gz": 2 * lax.rem(t, 2) + c}

    def remote(source, target, send, recv, device):
        return pltpu.make_async_remote_copy(
            src_ref=source, dst_ref=target, send_sem=send, recv_sem=recv, device_id=device, device_id_type=MESH
        )

    quarter = tall // SOURCE_PIECES
    load_src = lambda n: pltpu.make_async_copy(
        src.at[quarter * n : quarter * (n + 1), :], sbuf.at[quarter * n : quarter * (n + 1), :], src_sem.at[n]
    )
    group = lambda j: pl.ds(pl.multiple_of(wide * j, wide), wide)
    load_cos = lambda j: pltpu.make_async_copy(cos.at[:, group(j), :], ctab.at[:, group(j), :], cos_sem.at[j])
    loads = [
        pltpu.make_async_copy(a, b, in_sem.at[n])
        for n, (a, b) in enumerate(
            [(phi.at[kind], ptab), (edge.at[kind], etab), (lam, ltab), (lam_t.at[me], lttab), (modes, mtab)]
        )
    ]
    for n in range(SOURCE_PIECES):
        load_src(n).start()
    load_cos(0).start()
    for load in loads:
        load.start()
    for j in range(1, pairs):
        load_cos(j).start()
    for z in range(slab):
        wbuf[g, z : z + 1, :] = jnp.full((1, 128), width[z], jnp.float32)

    barrier = pltpu.get_barrier_semaphore()
    pl.semaphore_signal(barrier, inc=1, device_id=twin, device_id_type=MESH)
    pl.semaphore_signal(barrier, inc=1, device_id={"gz": 2 * (1 - h) + 1 - c}, device_id_type=MESH)
    for n in range(1, targets):
        pl.semaphore_signal(barrier, inc=1, device_id=at(lax.rem(me + n, targets)), device_id_type=MESH)
    pl.semaphore_wait(barrier, targets + 1)

    widths = lambda n, who: remote(wbuf.at[who], wbuf.at[who], w_send.at[n - 1], w_recv.at[who], {"gz": lax.rem(g + n, 4)})
    for n in range(1, 4):
        widths(n, g).start()

    for n in range(SOURCE_PIECES):
        load_src(n).wait()
        r = slice(quarter * n, quarter * (n + 1))
        s16[0, r, :], s16[1, r, :] = halves(sbuf[r, :])

    swap = lambda j: remote(xb.at[2 * j + 1 - c], rx.at[j], d_send.at[j], d_recv.at[j], twin)
    swap_a = lambda j: remote(amine.at[j], apeer.at[j], a_send.at[j], a_recv.at[j], across)
    swap_u = lambda j, who: remote(uo.at[j], xo.at[2 * j + who], u_send.at[j], u_recv.at[j], twin)
    piece = lambda t: pl.ds(pl.multiple_of(part * t, part), part)
    send_x = lambda j, n, t, who: remote(
        et.at[j, piece(t), :], rb.at[j, who], x_send.at[j, n - 1], x_recv.at[j, who], at(t)
    )
    send_y = lambda j, n, t, who: remote(msg.at[j, lax.div(t, 2)], rb2.at[j, who], y_send.at[j, n - 1], y_recv.at[j, who], at(t))
    peer_of = lambda n: lax.rem(me + n, targets)
    zero = jnp.zeros((part, 128), jnp.float32)
    lane = lax.broadcasted_iota(jnp.int32, (part, 128), 1)
    total = 4 * slab
    tiles = mtab.shape[1] // 128

    def cell(zz, side):
        zc = zz + side * (depth - 1 - 2 * zz)
        z = depth * side + zc
        row = pl.ds(z, 1)
        return zc, z, cf[side, row, :], cf[1 - side, row, :], cf[2, row, :]

    def along_x(j):
        load_cos(j).wait()
        dot = lambda a, b: lax.dot_general(s16[a], ctab[b, group(j), :], NT, preferred_element_type=jnp.float32)
        product = dot(0, 0) + dot(1, 0) + dot(0, 1)
        xb[2 * j] = product[:, :128]
        xb[2 * j + 1] = product[:, 128:]
        swap(j).start()

    def coefficients():
        for n in range(1, 4):
            widths(n, lax.rem(g + n, 4)).wait_recv()
        w = wbuf[...].reshape(total, 128)
        z = lax.broadcasted_iota(jnp.int32, (total, 128), 0)
        cf[0] = 2.0 / (w + jnp.where(z == 0, 0.0, pltpu.roll(w, 1, 0)))
        cf[1] = 2.0 / (w + jnp.where(z == total - 1, 0.0, pltpu.roll(w, total - 1, 0)))
        cf[2] = w
        for load in loads:
            load.wait()
        for n in range(3):
            bc[n] = jnp.broadcast_to(etab[:, n : n + 1], (rows, 128))
        for n in range(half + 2):
            mb[n] = jnp.broadcast_to(mtab[n : n + 1, :], (8, mtab.shape[1]))
        eb[lanes:, :] = jnp.zeros((128 - lanes, 128), jnp.float32)

    def transform(which, a, b):
        hi, lo = halves(jnp.concatenate([a, b], axis=1))
        both = lax.dot_general(
            ptab[which], jnp.concatenate([hi, lo], axis=0), NN, preferred_element_type=jnp.float32
        )
        both = both[:rows] + both[rows:]
        return both[:, :128], both[:, 128:]

    def first(j):
        eigen = bc[0] + ltab[pl.ds(2 * j + c, 1), :]
        ratios = [jnp.zeros((rows, 128), jnp.float32)] * 2
        for zz in range(depth):
            for n, (side, keep) in enumerate([(h, inv), (1 - h, inv2)]):
                zc, _z, outer, inner, w = cell(zz, side)
                inverse = 1.0 / ((outer + inner) + w * eigen - outer * ratios[n])
                keep[j, zc] = inverse
                ratios[n] = inner * inverse
        cmine[j], cpeer[j] = ratios
        join[j] = 1.0 / (1.0 - ratios[0] * ratios[1])
        for n in range(2):
            if n:
                swap(j).wait_recv()
            for zl in range(0, slab, 2):
                a, b = (slice(rows * y, rows * (y + 1)) for y in (zl, zl + 1))
                block = rx.at[j] if n else xb.at[2 * j + c]
                zc = slab * ((1 - c) if n else c) + zl
                fh[j, zc], fh[j, zc + 1] = transform(0, block[a, :], block[b, :])
        value = jnp.zeros((rows, 128), jnp.float32)
        for zz in range(depth):
            zc, _z, outer, _inner, w = cell(zz, h)
            value = (w * fh[j, zc] + outer * value) * inv[j, zc]
            vv[j, zc] = value
        amine[j] = value
        swap_a(j).start()

    def first_back(j):
        x = amine[j] * join[j]
        y = cpeer[j] * x
        for zz in reversed(range(depth)):
            zc, z, _outer, inner, _w = cell(zz, h)
            yc, yz, _outer, across_in, _w = cell(zz, 1 - h)
            if zz < depth - 1:
                x = vv[j, zc] + inner * inv[j, zc] * x
                y = across_in * inv2[j, yc] * y
            for n in range(2):
                eb[pl.ds(2 * depth * n + z, 1), :] = jnp.sum(bc[1 + n] * x, axis=0, keepdims=True)
                eb[pl.ds(2 * depth * n + yz, 1), :] = jnp.sum(bc[1 + n] * y, axis=0, keepdims=True)
        et[j] = jnp.transpose(eb[...])[:, :lanes]
        for n in range(1, targets):
            send_x(j, n, peer_of(n), me).start()
        rb[j, me] = et[j, piece(me), :]

    def cut_factors():
        eigen_k = [
            jnp.broadcast_to(jnp.sum(jnp.where(lane == 2 * j + c, lttab[...], 0.0), axis=1, keepdims=True), (part, 128))
            for j in range(pairs)
        ]

        def cut_factor(z, ratio):
            row = pl.ds(z, 1)
            lower, upper, w = cf[0, row, :], cf[1, row, :], cf[2, row, :]
            after = []
            for j in range(pairs):
                for q in range(tiles):
                    col = slice(128 * q, 128 * q + 128)
                    inverse = 1.0 / ((lower + upper) + w * (eigen_k[j] + mb[0, :, col]) - lower * ratio[j * tiles + q])
                    ginv[j, z, :, col] = inverse
                    after.append(upper * inverse)
            return tuple(after)

        lax.fori_loop(0, total, cut_factor, (zero,) * (pairs * tiles))

    def head(step, carry):
        @pl.when(step < pairs)
        def _():
            along_x(step)

        @pl.when(step == 1)
        def _():
            coefficients()

        @pl.when(step >= 1)
        def _():
            first(step - 1)
            first_back(step - 1)

        return carry

    lax.fori_loop(0, pairs + 1, head, 0)
    cut_factors()

    terms = lambda q: range(half) if q < tiles // 2 else range(half, cuts)
    mode = lambda m: 1 + (m if m < half else m - half)

    def cut(j, carry):
        for n in range(1, targets):
            t = peer_of(n)
            send_x(j, n, t, t).wait_recv()
        edge = [rb[j, 2 * i] + rb[j, 2 * i + 1] for i in range(parts)]
        jump = [edge[i][:, 2 * depth :] - edge[i + 1][:, : 2 * depth] for i in range(cuts)]
        mixed = [jump[i] - jump[cuts - 1 - i] for i in range(half)]
        mixed += [jump[i] + jump[cuts - 1 - i] for i in range(half)] + [jump[half]]
        for i in range(cuts):
            gt[i, :, : 2 * depth] = jump[i]
        value = [zero] * tiles
        for z in range(total):
            lower, w = cf[0, z : z + 1, :], cf[2, z : z + 1, :]
            force = [w * jnp.broadcast_to(m[:, z : z + 1], (part, 128)) for m in mixed]
            for q in range(tiles):
                col = slice(128 * q, 128 * q + 128)
                rhs = lower * value[q]
                for m in terms(q):
                    rhs = rhs + force[m] * mb[mode(m), :, col]
                value[q] = rhs * ginv[j, z, :, col]
                gv[z, :, col] = value[q]

        x = [zero] * tiles
        sums = [zero] * cuts
        for z in reversed(range(total)):
            upper = cf[1, z : z + 1, :]
            along = [zero] * cuts
            for q in range(tiles):
                col = slice(128 * q, 128 * q + 128)
                x[q] = gv[z, :, col] + upper * ginv[j, z, :, col] * x[q]
                for m in terms(q):
                    along[m] = along[m] + mb[mode(m), :, col] * x[q]
            for m in range(cuts):
                sums[m] = jnp.where(lane == z, jnp.sum(along[m], axis=1, keepdims=True), sums[m])
        true = [zero] * cuts
        for i in range(half):
            true[i] = gt[i] - (sums[half + i] + sums[i])
            true[cuts - 1 - i] = gt[cuts - 1 - i] - (sums[half + i] - sums[i])
        true[half] = gt[half] - sums[cuts - 1]
        for q in range(parts):
            left = true[q - 1] if q else zero
            right = pltpu.roll(true[q], 2 * depth, 1) if q < parts - 1 else zero
            msg[j, q] = (left + right)[:, :lanes]
        for n in range(1, targets):
            send_y(j, n, peer_of(n), me).start()
        rb2[j, me] = msg[j, p]
        return carry

    gt[...] = jnp.zeros(gt.shape, jnp.float32)
    lax.fori_loop(0, pairs, cut, 0)

    def second(j):
        for n in range(1, targets):
            t = peer_of(n)
            send_y(j, n, t, t).wait_recv()
        e2[...] = jnp.transpose(rb2[j].reshape(128, lanes))
        value = jnp.zeros((rows, 128), jnp.float32)
        other = value
        for zz in range(depth):
            zc, z, outer, _inner, w = cell(zz, h)
            left, right = e2[pl.ds(z, 1), :], e2[pl.ds(2 * depth + z, 1), :]
            force = fh[j, zc] + bc[1] * left - bc[2] * right
            value = (w * force + outer * value) * inv[j, zc]
            vv[j, zc] = value
            zc, z, outer, _inner, w = cell(zz, 1 - h)
            left, right = e2[pl.ds(z, 1), :], e2[pl.ds(2 * depth + z, 1), :]
            other = (w * (bc[1] * left - bc[2] * right) + outer * other) * inv2[j, zc]
        swap_a(j).wait_recv()
        x = (value + cmine[j] * (apeer[j] + other)) * join[j]
        for zz in reversed(range(depth)):
            zc, _z, _outer, inner, _w = cell(zz, h)
            if zz < depth - 1:
                x = vv[j, zc] + inner * inv[j, zc] * x
            fh[j, zc] = x
        for n in range(2):
            for zl in range(0, slab, 2):
                a, b = (slice(rows * y, rows * (y + 1)) for y in (zl, zl + 1))
                zc = slab * (c if n else (1 - c)) + zl
                block = xo.at[2 * j + c] if n else uo.at[j]
                block[a, :], block[b, :] = transform(1, fh[j, zc], fh[j, zc + 1])
            if n == 0:
                swap_u(j, c).start()

    def back_x(j):
        swap_u(j, 1 - c).wait_recv()
        for n in range(2):
            s16[0, :, 128 * n : 128 * n + 128], s16[1, :, 128 * n : 128 * n + 128] = halves(xo[2 * j + n])
        for n in range(pairs):
            i = slice(wide * n, wide * (n + 1))
            dot = lambda a, b: lax.dot_general(
                s16[a, :, :wide], ctab[b, group(j), i], NN, preferred_element_type=jnp.float32
            )
            out[:, i] = out[:, i] + (dot(0, 0) + dot(1, 0) + dot(0, 1))

    def tail(step, carry):
        @pl.when(step < pairs)
        def _():
            second(step)

        @pl.when(step >= 1)
        def _():
            back_x(step - 1)

        return carry

    out[...] = jnp.zeros(out.shape, jnp.float32)
    lax.fori_loop(0, pairs + 1, tail, 0)

    for n in range(1, 4):
        widths(n, g).wait_send()
    for j in range(pairs):
        for n in range(1, targets):
            send_x(j, n, peer_of(n), me).wait_send()
            send_y(j, n, peer_of(n), me).wait_send()
        swap(j).wait_send()
        swap_a(j).wait_send()
        swap_u(j, c).wait_send()


def fused(source, cell_width):
    slab, rows, nx = source.shape
    parts = lax.axis_size("pa")
    pairs, depth, targets = nx // 256, 2 * slab, 2 * parts
    part = 128 // targets
    ny = rows * parts
    consts = tables(nx, ny, parts, depth)
    f32, b16, V = jnp.float32, jnp.bfloat16, pltpu.VMEM
    tall = slab * rows
    lines = (pairs, depth, rows, 128)
    plane = (pairs, rows, 128)
    sem = lambda *n: pltpu.SemaphoreType.DMA(n)
    lanes = 4 * depth
    small = (pairs, targets, part, lanes)
    scratch = [
        V((tall, nx), f32), V((2, tall, nx), b16), V((2, nx, nx), b16), V((2, 2 * rows, 2 * rows), b16), V((rows, 128), f32),
        V(consts[3].shape, f32), V((part, 128), f32), V(consts[5].shape, f32), V((4, slab, 128), f32),
        V((3, 4 * slab, 128), f32), V((3, rows, 128), f32),
        V((2 * pairs, tall, 128), f32), V((pairs, tall, 128), f32), V(lines, f32), V(lines, f32), V(lines, f32),
        V(lines, f32), V(plane, f32), V(plane, f32), V(plane, f32), V(plane, f32), V(plane, f32),
        V((128, 128), f32), V((pairs, 128, lanes), f32), V(small, f32), V((parts, part, 128), f32),
        V((parts // 2 + 1, 8, ny), f32), V((pairs, 2 * depth, part, ny), f32), V((2 * depth, part, ny), f32),
        V((pairs, parts, part, lanes), f32), V(small, f32), V((lanes, 128), f32),
        V((pairs, tall, 128), f32), V((2 * pairs, tall, 128), f32),
        sem(5), sem(SOURCE_PIECES), sem(pairs), sem(3), sem(4), sem(pairs), sem(pairs),
        sem(pairs), sem(pairs), sem(pairs, targets), sem(pairs, targets), sem(pairs, targets), sem(pairs, targets),
        sem(pairs), sem(pairs),
    ]
    hbm = pl.BlockSpec(memory_space=pltpu.HBM)
    out = pl.pallas_call(
        functools.partial(fused_kernel, (parts, slab, rows, depth, pairs, part)),
        out_shape=pltpu.VMEM((tall, nx), f32),
        in_specs=[hbm, pl.BlockSpec(memory_space=pltpu.SMEM)] + [hbm] * 6,
        out_specs=pl.BlockSpec(memory_space=pltpu.VMEM),
        scratch_shapes=scratch,
        compiler_params=pltpu.CompilerParams(
            collective_id=0, has_side_effects=True, vmem_limit_bytes=60 * 1024 * 1024
        ),
    )(source.reshape(tall, nx), cell_width, *(jnp.asarray(t) for t in consts))
    return out.reshape(slab, rows, nx)


def fits(source, parts, blocks):
    slab, rows, nx = source.shape
    return (
        blocks == 4 and parts == 8 and nx % 256 == 0 and slab == 8 and rows % 16 == 0
        and (rows * parts) % 256 == 0
    )


def per_device(source, cell_width):
    if fits(source, lax.axis_size("pa"), lax.axis_size("gz")):
        return fused(source, cell_width)
    return on_device(source, cell_width)


def solution(mesh):
    in_specs = (P("gz", "pa", None), P("gz"))
    out_specs = P("gz", "pa", None)
    return jax.shard_map(
        per_device, mesh=mesh, in_specs=in_specs, out_specs=out_specs, check_vma=False
    )
```

```python
import functools

import jax
import jax.numpy as jnp
import numpy as np
from jax import lax
from jax.experimental import pallas as pl
from jax.experimental.pallas import tpu as pltpu
from jax.sharding import PartitionSpec as P

HIGH = lax.Precision.HIGH


def summed_angles(width, coarse, fine, sine):
    f32 = lambda x: jnp.asarray(x.astype(np.float32))
    ca, sa = f32(np.cos(coarse))[:, None, :], f32(np.sin(coarse))[:, None, :]
    cb, sb = f32(np.cos(fine))[None, :, :], f32(np.sin(fine))[None, :, :]
    table = sa * cb + ca * sb if sine else ca * cb - sa * sb
    return table.reshape(width, width)


def split_steps(width):
    step = next(b for b in (32, 16, 8, 1) if width % b == 0)
    return np.arange(0, width, step, dtype=np.int64)[:, None], np.arange(step, dtype=np.int64)[:, None]


def cosine_table(width):
    odd = 2 * np.arange(width, dtype=np.int64)[None, :] + 1
    a, b = (k * odd % (4 * width) * (np.pi / (2 * width)) for k in split_steps(width))
    first = jnp.arange(width)[:, None] == 0
    weights = jnp.where(first, np.sqrt(1.0 / width), np.sqrt(2.0 / width)).astype(jnp.float32)
    return weights * summed_angles(width, a, b, False)


def sine_table(width):
    j = np.arange(1, width + 1, dtype=np.int64)[None, :]
    coarse, fine = split_steps(width)
    a, b = (l * j % (2 * (width + 1)) * (np.pi / (width + 1)) for l in (coarse, fine + 1))
    return np.float32(np.sqrt(2.0 / (width + 1))) * summed_angles(width, a, b, True)


def eigen_first(offset, count, width):
    values = 4.0 * np.sin(np.arange(width) * (np.pi / (2 * width))) ** 2
    return lax.dynamic_slice_in_dim(jnp.asarray(values, jnp.float32), offset, count)[:, None]


def eigen_second(width):
    values = 4.0 * np.sin(np.arange(1, width + 1) * (np.pi / (2 * (width + 1)))) ** 2
    return jnp.asarray(values, jnp.float32)[None, :]


def tiles(rows, width, body):
    lanes = 256 if width % 256 == 0 else width

    if rows % 8:
        for c in range(0, width, lanes):
            body(slice(0, rows), pl.ds(c, lanes))
        return

    def step(r, carry):
        row = pl.ds(pl.multiple_of(r * 8, 8), 8)
        for c in range(0, width, lanes):
            body(row, pl.ds(c, lanes))
        return carry

    lax.fori_loop(0, rows // 8, step, 0)


def ends_kernel(coef, ex, ey, spectral, ends):
    depth, rows, width = spectral.shape

    def body(row, col):
        eigen = ex[row, :] + ey[:, col]
        diag = [coef[0, z] + coef[1, z] + coef[2, z] * eigen for z in range(depth)]
        force = [coef[2, z] * spectral[z, row, col] for z in range(depth)]
        inverse = 1.0 / diag[0]
        value = force[0] * inverse
        other = 1.0 / diag[depth - 1]
        front = force[depth - 1] * other
        for z in range(1, depth):
            inverse = 1.0 / (diag[z] - (coef[0, z] * coef[1, z - 1]) * inverse)
            value = (force[z] + coef[0, z] * value) * inverse
            y = depth - 1 - z
            other = 1.0 / (diag[y] - (coef[1, y] * coef[0, y + 1]) * other)
            front = (force[y] + coef[1, y] * front) * other
        ends[0, row, col] = front
        ends[1, row, col] = value

    tiles(rows, width, body)


def reduced_kernel(coef, ex, ey, ends, sides):
    blocks = ends.shape[0] // 2
    rows, width = ends.shape[1:]
    depth = coef.shape[1] // blocks

    def body(row, col):
        eigen = ex[row, :] + ey[:, col]
        p = jnp.zeros_like(eigen)
        q = jnp.zeros_like(eigen)
        saved = []
        for b in range(blocks):
            s = b * depth
            diag = [coef[0, s + z] + coef[1, s + z] + coef[2, s + z] * eigen for z in range(depth)]
            inverse = 1.0 / diag[0]
            v1 = coef[0, s] * inverse
            other = 1.0 / diag[depth - 1]
            w0 = coef[1, s + depth - 1] * other
            for z in range(1, depth):
                inverse = 1.0 / (diag[z] - (coef[0, s + z] * coef[1, s + z - 1]) * inverse)
                v1 = v1 * (coef[0, s + z] * inverse)
                y = depth - 1 - z
                other = 1.0 / (diag[y] - (coef[1, s + y] * coef[0, s + y + 1]) * other)
                w0 = w0 * (coef[1, s + y] * other)
            w1 = coef[1, s + depth - 1] * inverse
            v0 = coef[0, s] * other
            scale = 1.0 / (1.0 - v0 * q)
            a = (ends[2 * b, row, col] + v0 * p) * scale
            c = w0 * scale
            p, q = ends[2 * b + 1, row, col] + v1 * (p + q * a), v1 * q * c + w1
            saved.append((a, c, p, q))
        head = jnp.zeros_like(eigen)
        for b in reversed(range(blocks)):
            a, c, p, q = saved[b]
            sides[2 * b + 1, row, col] = head
            if b + 1 < blocks:
                sides[2 * b + 2, row, col] = p + q * head
            head = a + c * head
        sides[0, row, col] = jnp.zeros_like(eigen)

    tiles(rows, width, body)


def final_kernel(coef, ex, ey, spectral, sides, solved):
    depth, rows, width = spectral.shape

    def body(row, col):
        eigen = ex[row, :] + ey[:, col]
        ratios, values = [], []
        for z in range(depth):
            diag = coef[0, z] + coef[1, z] + coef[2, z] * eigen
            force = coef[2, z] * spectral[z, row, col]
            if z == 0:
                force = force + coef[0, z] * sides[0, row, col]
            else:
                diag = diag - coef[0, z] * ratios[-1]
                force = force + coef[0, z] * values[-1]
            if z == depth - 1:
                force = force + coef[1, z] * sides[1, row, col]
            inverse = 1.0 / diag
            ratios.append(coef[1, z] * inverse)
            values.append(force * inverse)
        x = values[-1]
        solved[depth - 1, row, col] = x
        for z in reversed(range(depth - 1)):
            x = values[z] + ratios[z] * x
            solved[z, row, col] = x

    tiles(rows, width, body)


def solve_call(kernel, leads, lead_out, coef, ex, ey, *planes):
    rows, width = planes[0].shape[1:]
    block = next((b for b in (32, 24, 16, 8) if rows % b == 0), rows)
    spec = lambda lead: pl.BlockSpec((lead, block, width), lambda i: (0, i, 0))
    return pl.pallas_call(
        kernel,
        grid=(rows // block,),
        in_specs=[
            pl.BlockSpec(memory_space=pltpu.SMEM),
            pl.BlockSpec((block, 1), lambda i: (i, 0)),
            pl.BlockSpec((1, width), lambda i: (0, 0)),
        ]
        + [spec(lead) for lead in leads],
        out_specs=spec(lead_out),
        out_shape=jax.ShapeDtypeStruct((lead_out, rows, width), jnp.float32),
    )(coef, ex, ey, *planes)


def on_device(source, cell_width):
    depth, rows_local, width_x = source.shape
    blocks = lax.axis_size("gz")
    width_y = rows_local * lax.axis_size("pa")
    cos_table = cosine_table(width_x)
    sin_table = sine_table(width_y)
    block = lax.axis_index("gz")
    widths = lax.all_gather(cell_width, "gz", tiled=True)
    padded = jnp.pad(widths, 1)
    coef = jnp.stack(
        [2.0 / (padded[:-2] + widths), 2.0 / (widths + padded[2:]), widths]
    )
    own = lax.dynamic_slice_in_dim(coef, block * depth, depth, axis=1)
    along_x = jnp.einsum("zyi,ki->zky", source, cos_table, precision=HIGH)
    spectral = jnp.einsum(
        "zkj,lj->zkl",
        lax.all_to_all(along_x, "pa", split_axis=1, concat_axis=2, tiled=True),
        sin_table,
        precision=HIGH,
    )
    kx = spectral.shape[1]
    first = lax.axis_index("pa") * kx
    part = kx // blocks
    ex = eigen_first(first, kx, width_x)
    ex_part = eigen_first(first + block * part, part, width_x)
    ey = eigen_second(width_y)
    ends = solve_call(ends_kernel, (depth,), 2, own, ex, ey, spectral)
    ends = lax.all_to_all(ends, "gz", split_axis=1, concat_axis=0, tiled=True)
    sides = solve_call(reduced_kernel, (2 * blocks,), 2 * blocks, coef, ex_part, ey, ends)
    sides = lax.all_to_all(sides, "gz", split_axis=0, concat_axis=1, tiled=True)
    solved = solve_call(final_kernel, (depth, 2), depth, own, ex, ey, spectral, sides)
    along_y = jnp.einsum("zkl,lj->zkj", solved, sin_table, precision=HIGH)
    return jnp.einsum(
        "zky,ki->zyi",
        lax.all_to_all(along_y, "pa", split_axis=2, concat_axis=1, tiled=True),
        cos_table,
        precision=HIGH,
    )


MESH = pl.DeviceIdType.MESH
NT = (((1,), (1,)), ((), ()))
NN = (((1,), (0,)), ((), ()))
SOURCE_PIECES = 4


def halves(x):
    hi = x.astype(jnp.bfloat16)
    return hi, (x - hi.astype(jnp.float32)).astype(jnp.bfloat16)


def block_modes(rows, kind):
    j, l = np.arange(rows), np.arange(rows)[:, None]
    if kind == 1:
        scale = np.sqrt(np.where(l == 0, 1.0, 2.0) / rows)
        angle = np.pi * l / rows
        vectors = scale * np.cos(angle * (2 * j + 1) / 2)
    else:
        angle = (2 * l + 1) * np.pi / (2 * rows + 1)
        vectors = 2.0 / np.sqrt(2 * rows + 1) * np.sin(angle * (j + 1))
    order = np.concatenate([j[::2], j[1::2]])
    vectors, values = vectors[order], 4.0 * np.sin(angle[order, 0] / 2) ** 2
    if kind == 2:
        vectors = vectors[:, ::-1]
    edge = vectors[:, 0] if kind else vectors[:, -1] * np.where(np.arange(rows) < rows // 2, 1.0, -1.0)
    return vectors, values, edge


def stacked(table):
    hi = table.astype(jnp.bfloat16)
    lo = (table - np.asarray(hi, np.float64)).astype(jnp.bfloat16)
    return np.block([[hi, hi], [lo, np.zeros_like(lo)]])


def tables(width, height, parts, depth):
    k, i = np.arange(width)[:, None], np.arange(width)[None, :]
    cos = np.sqrt(np.where(k == 0, 1.0, 2.0) / width) * np.cos(np.pi * (k * (2 * i + 1) % (4 * width)) / (2 * width))
    cos_hi = cos.astype(jnp.bfloat16)
    cos_lo = (cos - np.asarray(cos_hi, np.float64)).astype(jnp.bfloat16)
    rows = height // parts
    phi, edge = [], np.zeros((3, rows, 128), np.float32)
    for kind in range(3):
        vectors, values, ends = block_modes(rows, kind)
        phi.append(np.stack([stacked(vectors), stacked(vectors.T)]))
        edge[kind, :, 0], edge[kind, :, 1] = values, ends
    lam = (4.0 * np.sin(np.arange(width) * np.pi / (2 * width)) ** 2).astype(np.float32).reshape(-1, 128)
    groups = lam.shape[0]
    targets = 2 * parts
    lam_t = np.zeros((targets, 128 // targets, 128), np.float32)
    lam_t[:, :, :groups] = lam.T.reshape(targets, 128 // targets, groups)
    lam = np.pad(lam, ((0, -groups % 8), (0, 0)))
    l = np.arange(1, height + 1)
    l = np.concatenate([l[::2], l[1::2]])[None, :]
    cut = (np.arange(1, parts // 2 + 1) * rows)[:, None]
    sine = lambda j: np.sqrt(2.0 / (height + 1)) * np.sin(np.pi * (l * j % (2 * (height + 1))) / (height + 1))
    modes = np.concatenate([4.0 * np.sin(np.pi * l / (2 * (height + 1))) ** 2, sine(cut) - sine(cut + 1)])
    modes = np.pad(modes, ((0, -len(modes) % 8), (0, 0))).astype(np.float32)
    return np.stack([cos_hi, cos_lo]), np.stack(phi), edge, lam, lam_t, modes


def fused_kernel(
    size, src, width, cos, phi, edge, lam, lam_t, modes, out,
    sbuf, s16, ctab, ptab, etab, ltab, lttab, mtab, wbuf, cf, bc, xb, rx, fh, inv, vv, ratio,
    ratio2, cmine, cpeer, join, ends2, amine, apeer, eb, et, rb, gt, mb, ginv, gratio, gv, msg, rb2, e2, uo, xo,
    in_sem, src_sem, cos_sem, w_send, w_recv, d_send, d_recv, a_send, a_recv,
    x_send, x_recv, y_send, y_recv, u_send, u_recv,
):
    parts, slab, rows, depth, pairs, part = size
    targets = 2 * parts
    wide, lanes = 256, 4 * depth
    tall = slab * rows
    cuts, half = parts - 1, (parts - 1) // 2
    p, g = lax.axis_index("pa"), lax.axis_index("gz")
    h, c = lax.div(g, 2), lax.rem(g, 2)
    me = 2 * p + h
    kind = jnp.where(p == 0, 0, jnp.where(p == parts - 1, 2, 1))
    twin = {"gz": 2 * h + 1 - c}
    across = {"gz": 2 * (1 - h) + c}
    at = lambda t: {"pa": lax.div(t, 2), "gz": 2 * lax.rem(t, 2) + 1 - c}

    def remote(source, target, send, recv, device):
        return pltpu.make_async_remote_copy(
            src_ref=source, dst_ref=target, send_sem=send, recv_sem=recv, device_id=device, device_id_type=MESH
        )

    quarter = tall // SOURCE_PIECES
    load_src = lambda n: pltpu.make_async_copy(
        src.at[quarter * n : quarter * (n + 1), :], sbuf.at[quarter * n : quarter * (n + 1), :], src_sem.at[n]
    )
    group = lambda j: pl.ds(pl.multiple_of(wide * j, wide), wide)
    load_cos = lambda j: pltpu.make_async_copy(cos.at[:, group(j), :], ctab.at[:, group(j), :], cos_sem.at[j])
    loads = [
        pltpu.make_async_copy(a, b, in_sem.at[n])
        for n, (a, b) in enumerate(
            [(phi.at[kind], ptab), (edge.at[kind], etab), (lam, ltab), (lam_t.at[me], lttab), (modes, mtab)]
        )
    ]
    for n in range(SOURCE_PIECES):
        load_src(n).start()
    load_cos(0).start()
    for load in loads:
        load.start()
    for z in range(slab):
        wbuf[g, z : z + 1, :] = jnp.full((1, 128), width[z], jnp.float32)

    barrier = pltpu.get_barrier_semaphore()
    pl.semaphore_signal(barrier, inc=1, device_id=across, device_id_type=MESH)
    for n in range(targets):
        pl.semaphore_signal(barrier, inc=1, device_id=at(lax.rem(me + n, targets)), device_id_type=MESH)
    pl.semaphore_wait(barrier, targets + 1)

    widths = lambda n, who: remote(wbuf.at[who], wbuf.at[who], w_send.at[n - 1], w_recv.at[who], {"gz": lax.rem(g + n, 4)})
    for n in range(1, 4):
        widths(n, g).start()

    for n in range(SOURCE_PIECES):
        load_src(n).wait()
        if n == SOURCE_PIECES - 1:
            for j in range(1, pairs):
                load_cos(j).start()
        r = slice(quarter * n, quarter * (n + 1))
        s16[0, r, :], s16[1, r, :] = halves(sbuf[r, :])

    swap = lambda j: remote(xb.at[2 * j + 1 - c], rx.at[j], d_send.at[j], d_recv.at[j], twin)
    swap_a = lambda j: remote(amine.at[j], apeer.at[j], a_send.at[j], a_recv.at[j], across)
    swap_u = lambda j, who: remote(uo.at[j], xo.at[2 * j + who], u_send.at[j], u_recv.at[j], twin)
    piece = lambda t: pl.ds(pl.multiple_of(part * t, part), part)
    send_x = lambda j, n, t, who: remote(
        et.at[j, piece(t), :], rb.at[j, who], x_send.at[j, n], x_recv.at[j, who], at(t)
    )
    send_y = lambda j, n, t, who: remote(msg.at[j, lax.div(t, 2)], rb2.at[j, who], y_send.at[j, n], y_recv.at[j, who], at(t))
    peer_of = lambda n: lax.rem(me + n, targets)
    zero = jnp.zeros((part, 128), jnp.float32)
    lane = lax.broadcasted_iota(jnp.int32, (part, 128), 1)
    total = 4 * slab
    tiles = mtab.shape[1] // 128

    def cell(zz, side):
        zc = zz + side * (depth - 1 - 2 * zz)
        z = depth * side + zc
        row = pl.ds(z, 1)
        return zc, z, cf[side, row, :], cf[1 - side, row, :], cf[2, row, :]

    def along_x(j):
        load_cos(j).wait()
        dot = lambda a, b: lax.dot_general(s16[a], ctab[b, group(j), :], NT, preferred_element_type=jnp.float32)
        product = dot(0, 0) + dot(1, 0) + dot(0, 1)
        xb[2 * j] = product[:, :128]
        xb[2 * j + 1] = product[:, 128:]
        swap(j).start()

    def coefficients():
        for n in range(1, 4):
            widths(n, lax.rem(g + n, 4)).wait_recv()
        w = wbuf[...].reshape(total, 128)
        z = lax.broadcasted_iota(jnp.int32, (total, 128), 0)
        cf[0] = 2.0 / (w + jnp.where(z == 0, 0.0, pltpu.roll(w, 1, 0)))
        cf[1] = 2.0 / (w + jnp.where(z == total - 1, 0.0, pltpu.roll(w, total - 1, 0)))
        cf[2] = w
        for load in loads:
            load.wait()
        for n in range(2):
            bc[n] = jnp.broadcast_to(etab[:, n : n + 1], (rows, 128))
        for n in range(half + 2):
            mb[n] = jnp.broadcast_to(mtab[n : n + 1, :], (8, mtab.shape[1]))
        eb[lanes:, :] = jnp.zeros((128 - lanes, 128), jnp.float32)

    def transform(which, a, b):
        hi, lo = halves(jnp.concatenate([a, b], axis=1))
        both = lax.dot_general(
            ptab[which], jnp.concatenate([hi, lo], axis=0), NN, preferred_element_type=jnp.float32
        )
        both = both[:rows] + both[rows:]
        return both[:, :128], both[:, 128:]

    def first(j):
        eigen = bc[0] + ltab[pl.ds(2 * j + c, 1), :]
        ratios = [jnp.zeros((rows, 128), jnp.float32)] * 2
        for zz in range(depth):
            for n, (side, keep) in enumerate([(h, ratio), (1 - h, ratio2)]):
                zc, _z, outer, inner, w = cell(zz, side)
                inverse = 1.0 / ((outer + inner) + w * eigen - outer * ratios[n])
                ratios[n] = inner * inverse
                keep[j, zc] = ratios[n]
                if n == 0:
                    inv[j, zc] = inverse
        ends2[j] = inverse
        cmine[j], cpeer[j] = ratios
        join[j] = 1.0 / (1.0 - ratios[0] * ratios[1])
        for n in range(2):
            if n:
                swap(j).wait_recv()
            for zl in range(0, slab, 2):
                a, b = (slice(rows * y, rows * (y + 1)) for y in (zl, zl + 1))
                block = rx.at[j] if n else xb.at[2 * j + c]
                zc = slab * ((1 - c) if n else c) + zl
                z = depth * h + zc
                a, b = transform(0, block[a, :], block[b, :])
                fh[j, zc] = cf[2, pl.ds(z, 1), :] * a
                fh[j, zc + 1] = cf[2, pl.ds(z + 1, 1), :] * b
        for zz in range(depth):
            zc = cell(zz, h)[0]
            value = fh[j, zc] + ratio[j, before] * value if zz else fh[j, zc]
            vv[j, zc] = value
            before = zc
        value = value * inv[j, before]
        amine[j] = value
        swap_a(j).start()

    def first_back(j):
        x = amine[j] * join[j]
        y = cpeer[j] * x
        for zz in reversed(range(depth)):
            zc, z = cell(zz, h)[:2]
            yc, yz = cell(zz, 1 - h)[:2]
            if zz < depth - 1:
                x = vv[j, zc] * inv[j, zc] + ratio[j, zc] * x
                y = ratio2[j, yc] * y
            for at_z, plane in ((z, x), (yz, y)):
                weighted = bc[1] * plane
                for n in range(2):
                    rows_n = weighted[rows // 2 * n : rows // 2 * (n + 1)]
                    eb[pl.ds(2 * depth * n + at_z, 1), :] = jnp.sum(rows_n, axis=0, keepdims=True)
        et[j] = jnp.transpose(eb[...])[:, :lanes]
        for n in range(targets):
            send_x(j, n, peer_of(n), me).start()

    def cut_factors():
        eigen_k = [
            jnp.broadcast_to(jnp.sum(jnp.where(lane == 2 * j + 1 - c, lttab[...], 0.0), axis=1, keepdims=True), (part, 128))
            for j in range(pairs)
        ]

        def cut_factor(z, ratio):
            row = pl.ds(z, 1)
            lower, upper, w = cf[0, row, :], cf[1, row, :], cf[2, row, :]
            after = []
            for j in range(pairs):
                for q in range(tiles):
                    col = slice(128 * q, 128 * q + 128)
                    inverse = 1.0 / ((lower + upper) + w * (eigen_k[j] + mb[0, :, col]) - lower * ratio[j * tiles + q])
                    ginv[j, z, :, col] = inverse
                    after.append(upper * inverse)
                    gratio[j, z, :, col] = after[-1]
            return tuple(after)

        lax.fori_loop(0, total, cut_factor, (zero,) * (pairs * tiles))

    def head(step, carry):
        @pl.when(step < pairs)
        def _():
            along_x(step)

        @pl.when(step == 1)
        def _():
            coefficients()

        @pl.when(step >= 1)
        def _():
            first(step - 1)
            first_back(step - 1)

        return carry

    lax.fori_loop(0, pairs + 1, head, 0)
    cut_factors()

    terms = lambda q: range(half) if q < tiles // 2 else range(half, cuts)
    mode = lambda m: 1 + (m if m < half else m - half)

    def cut(j, carry):
        for n in range(targets):
            t = peer_of(n)
            send_x(j, n, t, t).wait_recv()
        edge = [rb[j, 2 * i] + rb[j, 2 * i + 1] for i in range(parts)]
        even, odd = ([e[:, k : k + 2 * depth] for e in edge] for k in (0, 2 * depth))
        jump = [(even[i] - even[i + 1]) - (odd[i] + odd[i + 1]) for i in range(cuts)]
        mixed = [jump[i] - jump[cuts - 1 - i] for i in range(half)]
        mixed += [jump[i] + jump[cuts - 1 - i] for i in range(half)] + [jump[half]]
        for i in range(cuts):
            gt[i, :, : 2 * depth] = jump[i]
        value = [zero] * tiles
        for z in range(total):
            w = cf[2, z : z + 1, :]
            force = [w * jnp.broadcast_to(m[:, z : z + 1], (part, 128)) for m in mixed]
            for q in range(tiles):
                col = slice(128 * q, 128 * q + 128)
                rhs = gratio[j, z - 1, :, col] * value[q] if z else zero
                for m in terms(q):
                    rhs = rhs + force[m] * mb[mode(m), :, col]
                value[q] = rhs
                gv[z, :, col] = rhs

        x = [zero] * tiles
        sums = [zero] * cuts
        for z in reversed(range(total)):
            along = [zero] * cuts
            for q in range(tiles):
                col = slice(128 * q, 128 * q + 128)
                x[q] = gv[z, :, col] * ginv[j, z, :, col] + gratio[j, z, :, col] * x[q]
                for m in terms(q):
                    along[m] = along[m] + mb[mode(m), :, col] * x[q]
            for m in range(cuts):
                sums[m] = jnp.where(lane == z, jnp.sum(along[m], axis=1, keepdims=True), sums[m])
        true = [zero] * cuts
        for i in range(half):
            true[i] = gt[i] - (sums[half + i] + sums[i])
            true[cuts - 1 - i] = gt[cuts - 1 - i] - (sums[half + i] - sums[i])
        true[half] = gt[half] - sums[cuts - 1]
        for q in range(parts):
            left = true[q - 1] if q else zero
            right = true[q] if q < parts - 1 else zero
            msg[j, q] = ((left - right) + pltpu.roll(left + right, 2 * depth, 1))[:, :lanes]
        for n in range(targets):
            send_y(j, n, peer_of(n), me).start()
        return carry

    gt[...] = jnp.zeros(gt.shape, jnp.float32)
    lax.fori_loop(0, pairs, cut, 0)

    def second(j):
        for n in range(targets):
            t = peer_of(n)
            send_y(j, n, t, t).wait_recv()
        e2[...] = jnp.transpose(rb2[j].reshape(128, lanes))
        def pull(z, w):
            mode_rows = [slice(rows // 2 * n, rows // 2 * (n + 1)) for n in range(2)]
            return jnp.concatenate([bc[1, r] * (w * e2[pl.ds(2 * depth * n + z, 1), :]) for n, r in enumerate(mode_rows)])

        for zz in range(depth):
            zc, z, _outer, _inner, w = cell(zz, h)
            force = fh[j, zc] + pull(z, w)
            value = force + ratio[j, before] * value if zz else force
            vv[j, zc] = value
            before = zc
            zc, z, _outer, _inner, w = cell(zz, 1 - h)
            force = pull(z, w)
            other = force + ratio2[j, before2] * other if zz else force
            before2 = zc
        swap_a(j).wait_recv()
        x = (value * inv[j, before] + cmine[j] * (apeer[j] + other * ends2[j])) * join[j]
        for zz in reversed(range(depth)):
            zc = cell(zz, h)[0]
            if zz < depth - 1:
                x = vv[j, zc] * inv[j, zc] + ratio[j, zc] * x
            fh[j, zc] = x
        for n in range(2):
            for zl in range(0, slab, 2):
                a, b = (slice(rows * y, rows * (y + 1)) for y in (zl, zl + 1))
                zc = slab * (c if n else (1 - c)) + zl
                block = xo.at[2 * j + c] if n else uo.at[j]
                block[a, :], block[b, :] = transform(1, fh[j, zc], fh[j, zc + 1])
            if n == 0:
                swap_u(j, c).start()

    def back_x(j):
        swap_u(j, 1 - c).wait_recv()
        for n in range(2):
            s16[0, :, 128 * n : 128 * n + 128], s16[1, :, 128 * n : 128 * n + 128] = halves(xo[2 * j + n])
        for n in range(pairs):
            i = slice(wide * n, wide * (n + 1))
            dot = lambda a, b: lax.dot_general(
                s16[a, :, :wide], ctab[b, group(j), i], NN, preferred_element_type=jnp.float32
            )
            out[:, i] = out[:, i] + (dot(0, 0) + dot(1, 0) + dot(0, 1))

    def tail(step, carry):
        @pl.when(step < pairs)
        def _():
            second(step)

        @pl.when(step >= 1)
        def _():
            back_x(step - 1)

        return carry

    out[...] = jnp.zeros(out.shape, jnp.float32)
    lax.fori_loop(0, pairs + 1, tail, 0)

    for n in range(1, 4):
        widths(n, g).wait_send()
    for j in range(pairs):
        for n in range(targets):
            send_x(j, n, peer_of(n), me).wait_send()
            send_y(j, n, peer_of(n), me).wait_send()
        swap(j).wait_send()
        swap_a(j).wait_send()
        swap_u(j, c).wait_send()


def fused(source, cell_width):
    slab, rows, nx = source.shape
    parts = lax.axis_size("pa")
    pairs, depth, targets = nx // 256, 2 * slab, 2 * parts
    part = 128 // targets
    ny = rows * parts
    consts = tables(nx, ny, parts, depth)
    f32, b16, V = jnp.float32, jnp.bfloat16, pltpu.VMEM
    tall = slab * rows
    lines = (pairs, depth, rows, 128)
    plane = (pairs, rows, 128)
    sem = lambda *n: pltpu.SemaphoreType.DMA(n)
    lanes = 4 * depth
    small = (pairs, targets, part, lanes)
    scratch = [
        V((tall, nx), f32), V((2, tall, nx), b16), V((2, nx, nx), b16), V((2, 2 * rows, 2 * rows), b16), V((rows, 128), f32),
        V(consts[3].shape, f32), V((part, 128), f32), V(consts[5].shape, f32), V((4, slab, 128), f32),
        V((3, 4 * slab, 128), f32), V((2, rows, 128), f32),
        V((2 * pairs, tall, 128), f32), V((pairs, tall, 128), f32), V(lines, f32), V(lines, f32), V(lines, f32), V(lines, f32),
        V(lines, f32), V(plane, f32), V(plane, f32), V(plane, f32), V(plane, f32), V(plane, f32), V(plane, f32),
        V((128, 128), f32), V((pairs, 128, lanes), f32), V(small, f32), V((parts, part, 128), f32),
        V((parts // 2 + 1, 8, ny), f32), V((pairs, 2 * depth, part, ny), f32), V((pairs, 2 * depth, part, ny), f32), V((2 * depth, part, ny), f32),
        V((pairs, parts, part, lanes), f32), V(small, f32), V((lanes, 128), f32),
        V((pairs, tall, 128), f32), V((2 * pairs, tall, 128), f32),
        sem(5), sem(SOURCE_PIECES), sem(pairs), sem(3), sem(4), sem(pairs), sem(pairs),
        sem(pairs), sem(pairs), sem(pairs, targets), sem(pairs, targets), sem(pairs, targets), sem(pairs, targets),
        sem(pairs), sem(pairs),
    ]
    hbm = pl.BlockSpec(memory_space=pltpu.HBM)
    out = pl.pallas_call(
        functools.partial(fused_kernel, (parts, slab, rows, depth, pairs, part)),
        out_shape=pltpu.VMEM((tall, nx), f32),
        in_specs=[hbm, pl.BlockSpec(memory_space=pltpu.SMEM)] + [hbm] * 6,
        out_specs=pl.BlockSpec(memory_space=pltpu.VMEM),
        scratch_shapes=scratch,
        compiler_params=pltpu.CompilerParams(
            collective_id=0, has_side_effects=True, vmem_limit_bytes=60 * 1024 * 1024
        ),
    )(source.reshape(tall, nx), cell_width, *(jnp.asarray(t) for t in consts))
    return out.reshape(slab, rows, nx)


def fits(source, parts, blocks):
    slab, rows, nx = source.shape
    return (
        blocks == 4 and parts == 8 and nx % 256 == 0 and slab == 8 and rows % 16 == 0
        and (rows * parts) % 256 == 0
    )


def per_device(source, cell_width):
    if fits(source, lax.axis_size("pa"), lax.axis_size("gz")):
        return fused(source, cell_width)
    return on_device(source, cell_width)


def solution(mesh):
    in_specs = (P("gz", "pa", None), P("gz"))
    out_specs = P("gz", "pa", None)
    return jax.shard_map(
        per_device, mesh=mesh, in_specs=in_specs, out_specs=out_specs, check_vma=False
    )
```

```python
import functools

import jax
import jax.numpy as jnp
import numpy as np
from jax import lax
from jax.experimental import pallas as pl
from jax.experimental.pallas import tpu as pltpu
from jax.sharding import PartitionSpec as P

HIGH = lax.Precision.HIGH


def summed_angles(width, coarse, fine, sine):
    f32 = lambda x: jnp.asarray(x.astype(np.float32))
    ca, sa = f32(np.cos(coarse))[:, None, :], f32(np.sin(coarse))[:, None, :]
    cb, sb = f32(np.cos(fine))[None, :, :], f32(np.sin(fine))[None, :, :]
    table = sa * cb + ca * sb if sine else ca * cb - sa * sb
    return table.reshape(width, width)


def split_steps(width):
    step = next(b for b in (32, 16, 8, 1) if width % b == 0)
    return np.arange(0, width, step, dtype=np.int64)[:, None], np.arange(step, dtype=np.int64)[:, None]


def cosine_table(width):
    odd = 2 * np.arange(width, dtype=np.int64)[None, :] + 1
    a, b = (k * odd % (4 * width) * (np.pi / (2 * width)) for k in split_steps(width))
    first = jnp.arange(width)[:, None] == 0
    weights = jnp.where(first, np.sqrt(1.0 / width), np.sqrt(2.0 / width)).astype(jnp.float32)
    return weights * summed_angles(width, a, b, False)


def sine_table(width):
    j = np.arange(1, width + 1, dtype=np.int64)[None, :]
    coarse, fine = split_steps(width)
    a, b = (l * j % (2 * (width + 1)) * (np.pi / (width + 1)) for l in (coarse, fine + 1))
    return np.float32(np.sqrt(2.0 / (width + 1))) * summed_angles(width, a, b, True)


def eigen_first(offset, count, width):
    values = 4.0 * np.sin(np.arange(width) * (np.pi / (2 * width))) ** 2
    return lax.dynamic_slice_in_dim(jnp.asarray(values, jnp.float32), offset, count)[:, None]


def eigen_second(width):
    values = 4.0 * np.sin(np.arange(1, width + 1) * (np.pi / (2 * (width + 1)))) ** 2
    return jnp.asarray(values, jnp.float32)[None, :]


def tiles(rows, width, body):
    lanes = 256 if width % 256 == 0 else width

    if rows % 8:
        for c in range(0, width, lanes):
            body(slice(0, rows), pl.ds(c, lanes))
        return

    def step(r, carry):
        row = pl.ds(pl.multiple_of(r * 8, 8), 8)
        for c in range(0, width, lanes):
            body(row, pl.ds(c, lanes))
        return carry

    lax.fori_loop(0, rows // 8, step, 0)


def ends_kernel(coef, ex, ey, spectral, ends):
    depth, rows, width = spectral.shape

    def body(row, col):
        eigen = ex[row, :] + ey[:, col]
        diag = [coef[0, z] + coef[1, z] + coef[2, z] * eigen for z in range(depth)]
        force = [coef[2, z] * spectral[z, row, col] for z in range(depth)]
        inverse = 1.0 / diag[0]
        value = force[0] * inverse
        other = 1.0 / diag[depth - 1]
        front = force[depth - 1] * other
        for z in range(1, depth):
            inverse = 1.0 / (diag[z] - (coef[0, z] * coef[1, z - 1]) * inverse)
            value = (force[z] + coef[0, z] * value) * inverse
            y = depth - 1 - z
            other = 1.0 / (diag[y] - (coef[1, y] * coef[0, y + 1]) * other)
            front = (force[y] + coef[1, y] * front) * other
        ends[0, row, col] = front
        ends[1, row, col] = value

    tiles(rows, width, body)


def reduced_kernel(coef, ex, ey, ends, sides):
    blocks = ends.shape[0] // 2
    rows, width = ends.shape[1:]
    depth = coef.shape[1] // blocks

    def body(row, col):
        eigen = ex[row, :] + ey[:, col]
        p = jnp.zeros_like(eigen)
        q = jnp.zeros_like(eigen)
        saved = []
        for b in range(blocks):
            s = b * depth
            diag = [coef[0, s + z] + coef[1, s + z] + coef[2, s + z] * eigen for z in range(depth)]
            inverse = 1.0 / diag[0]
            v1 = coef[0, s] * inverse
            other = 1.0 / diag[depth - 1]
            w0 = coef[1, s + depth - 1] * other
            for z in range(1, depth):
                inverse = 1.0 / (diag[z] - (coef[0, s + z] * coef[1, s + z - 1]) * inverse)
                v1 = v1 * (coef[0, s + z] * inverse)
                y = depth - 1 - z
                other = 1.0 / (diag[y] - (coef[1, s + y] * coef[0, s + y + 1]) * other)
                w0 = w0 * (coef[1, s + y] * other)
            w1 = coef[1, s + depth - 1] * inverse
            v0 = coef[0, s] * other
            scale = 1.0 / (1.0 - v0 * q)
            a = (ends[2 * b, row, col] + v0 * p) * scale
            c = w0 * scale
            p, q = ends[2 * b + 1, row, col] + v1 * (p + q * a), v1 * q * c + w1
            saved.append((a, c, p, q))
        head = jnp.zeros_like(eigen)
        for b in reversed(range(blocks)):
            a, c, p, q = saved[b]
            sides[2 * b + 1, row, col] = head
            if b + 1 < blocks:
                sides[2 * b + 2, row, col] = p + q * head
            head = a + c * head
        sides[0, row, col] = jnp.zeros_like(eigen)

    tiles(rows, width, body)


def final_kernel(coef, ex, ey, spectral, sides, solved):
    depth, rows, width = spectral.shape

    def body(row, col):
        eigen = ex[row, :] + ey[:, col]
        ratios, values = [], []
        for z in range(depth):
            diag = coef[0, z] + coef[1, z] + coef[2, z] * eigen
            force = coef[2, z] * spectral[z, row, col]
            if z == 0:
                force = force + coef[0, z] * sides[0, row, col]
            else:
                diag = diag - coef[0, z] * ratios[-1]
                force = force + coef[0, z] * values[-1]
            if z == depth - 1:
                force = force + coef[1, z] * sides[1, row, col]
            inverse = 1.0 / diag
            ratios.append(coef[1, z] * inverse)
            values.append(force * inverse)
        x = values[-1]
        solved[depth - 1, row, col] = x
        for z in reversed(range(depth - 1)):
            x = values[z] + ratios[z] * x
            solved[z, row, col] = x

    tiles(rows, width, body)


def solve_call(kernel, leads, lead_out, coef, ex, ey, *planes):
    rows, width = planes[0].shape[1:]
    block = next((b for b in (32, 24, 16, 8) if rows % b == 0), rows)
    spec = lambda lead: pl.BlockSpec((lead, block, width), lambda i: (0, i, 0))
    return pl.pallas_call(
        kernel,
        grid=(rows // block,),
        in_specs=[
            pl.BlockSpec(memory_space=pltpu.SMEM),
            pl.BlockSpec((block, 1), lambda i: (i, 0)),
            pl.BlockSpec((1, width), lambda i: (0, 0)),
        ]
        + [spec(lead) for lead in leads],
        out_specs=spec(lead_out),
        out_shape=jax.ShapeDtypeStruct((lead_out, rows, width), jnp.float32),
    )(coef, ex, ey, *planes)


def on_device(source, cell_width):
    depth, rows_local, width_x = source.shape
    blocks = lax.axis_size("gz")
    width_y = rows_local * lax.axis_size("pa")
    cos_table = cosine_table(width_x)
    sin_table = sine_table(width_y)
    block = lax.axis_index("gz")
    widths = lax.all_gather(cell_width, "gz", tiled=True)
    padded = jnp.pad(widths, 1)
    coef = jnp.stack(
        [2.0 / (padded[:-2] + widths), 2.0 / (widths + padded[2:]), widths]
    )
    own = lax.dynamic_slice_in_dim(coef, block * depth, depth, axis=1)
    along_x = jnp.einsum("zyi,ki->zky", source, cos_table, precision=HIGH)
    spectral = jnp.einsum(
        "zkj,lj->zkl",
        lax.all_to_all(along_x, "pa", split_axis=1, concat_axis=2, tiled=True),
        sin_table,
        precision=HIGH,
    )
    kx = spectral.shape[1]
    first = lax.axis_index("pa") * kx
    part = kx // blocks
    ex = eigen_first(first, kx, width_x)
    ex_part = eigen_first(first + block * part, part, width_x)
    ey = eigen_second(width_y)
    ends = solve_call(ends_kernel, (depth,), 2, own, ex, ey, spectral)
    ends = lax.all_to_all(ends, "gz", split_axis=1, concat_axis=0, tiled=True)
    sides = solve_call(reduced_kernel, (2 * blocks,), 2 * blocks, coef, ex_part, ey, ends)
    sides = lax.all_to_all(sides, "gz", split_axis=0, concat_axis=1, tiled=True)
    solved = solve_call(final_kernel, (depth, 2), depth, own, ex, ey, spectral, sides)
    along_y = jnp.einsum("zkl,lj->zkj", solved, sin_table, precision=HIGH)
    return jnp.einsum(
        "zky,ki->zyi",
        lax.all_to_all(along_y, "pa", split_axis=2, concat_axis=1, tiled=True),
        cos_table,
        precision=HIGH,
    )


MESH = pl.DeviceIdType.MESH
NT = (((1,), (1,)), ((), ()))
NN = (((1,), (0,)), ((), ()))
SOURCE_PIECES = 4


def halves(x):
    hi = x.astype(jnp.bfloat16)
    return hi, (x - hi.astype(jnp.float32)).astype(jnp.bfloat16)


def block_modes(rows, kind):
    j, l = np.arange(rows), np.arange(rows)[:, None]
    if kind == 1:
        scale = np.sqrt(np.where(l == 0, 1.0, 2.0) / rows)
        angle = np.pi * l / rows
        vectors = scale * np.cos(angle * (2 * j + 1) / 2)
    else:
        angle = (2 * l + 1) * np.pi / (2 * rows + 1)
        vectors = 2.0 / np.sqrt(2 * rows + 1) * np.sin(angle * (j + 1))
    order = np.concatenate([j[::2], j[1::2]])
    vectors, values = vectors[order], 4.0 * np.sin(angle[order, 0] / 2) ** 2
    if kind == 2:
        vectors = vectors[:, ::-1]
    edge = vectors[:, 0] if kind else vectors[:, -1] * np.where(np.arange(rows) < rows // 2, 1.0, -1.0)
    return vectors, values, edge


def stacked(table):
    hi = table.astype(jnp.bfloat16)
    lo = (table - np.asarray(hi, np.float64)).astype(jnp.bfloat16)
    return np.block([[hi, hi], [lo, np.zeros_like(lo)]])


def tables(width, height, parts, depth):
    k, i = np.arange(width)[:, None], np.arange(width)[None, :]
    cos = np.sqrt(np.where(k == 0, 1.0, 2.0) / width) * np.cos(np.pi * (k * (2 * i + 1) % (4 * width)) / (2 * width))
    cos_hi = cos.astype(jnp.bfloat16)
    cos_lo = (cos - np.asarray(cos_hi, np.float64)).astype(jnp.bfloat16)
    rows = height // parts
    phi, edge = [], np.zeros((3, rows, 128), np.float32)
    for kind in range(3):
        vectors, values, ends = block_modes(rows, kind)
        phi.append(np.stack([stacked(vectors), stacked(vectors.T)]))
        edge[kind, :, 0], edge[kind, :, 1] = values, ends
    lam = (4.0 * np.sin(np.arange(width) * np.pi / (2 * width)) ** 2).astype(np.float32).reshape(-1, 128)
    groups = lam.shape[0]
    targets = 2 * parts
    lam_t = np.zeros((targets, 128 // targets, 128), np.float32)
    lam_t[:, :, :groups] = lam.T.reshape(targets, 128 // targets, groups)
    lam = np.pad(lam, ((0, -groups % 8), (0, 0)))
    l = np.arange(1, height + 1)
    l = np.concatenate([l[::2], l[1::2]])[None, :]
    cut = (np.arange(1, parts // 2 + 1) * rows)[:, None]
    sine = lambda j: np.sqrt(2.0 / (height + 1)) * np.sin(np.pi * (l * j % (2 * (height + 1))) / (height + 1))
    modes = np.concatenate([4.0 * np.sin(np.pi * l / (2 * (height + 1))) ** 2, sine(cut) - sine(cut + 1)])
    modes = np.pad(modes, ((0, -len(modes) % 8), (0, 0))).astype(np.float32)
    return np.stack([cos_hi, cos_lo]), np.stack(phi), edge, lam, lam_t, modes


def fused_kernel(
    size, src, width, cos, phi, edge, lam, lam_t, modes, out,
    sbuf, s16, ctab, ptab, etab, ltab, lttab, mtab, wbuf, cf, bc, xb, rx, fh, inv, vv, ratio,
    ratio2, cmine, cpeer, join, ends2, amine, apeer, eb, et, rb, gt, mb, ginv, gratio, gv, msg, rb2, e2, uo, xo,
    in_sem, src_sem, cos_sem, w_send, w_recv, d_send, d_recv, a_send, a_recv,
    x_send, x_recv, y_send, y_recv, u_send, u_recv,
):
    parts, slab, rows, depth, pairs, part = size
    targets = 2 * parts
    wide, lanes = 256, 4 * depth
    tall = slab * rows
    cuts, half = parts - 1, (parts - 1) // 2
    p, g = lax.axis_index("pa"), lax.axis_index("gz")
    h, c = lax.div(g, 2), lax.rem(g, 2)
    me = 2 * p + h
    kind = jnp.where(p == 0, 0, jnp.where(p == parts - 1, 2, 1))
    twin = {"gz": 2 * h + 1 - c}
    across = {"gz": 2 * (1 - h) + c}
    at = lambda t: {"pa": lax.div(t, 2), "gz": 2 * lax.rem(t, 2) + 1 - c}

    def remote(source, target, send, recv, device):
        return pltpu.make_async_remote_copy(
            src_ref=source, dst_ref=target, send_sem=send, recv_sem=recv, device_id=device, device_id_type=MESH
        )

    quarter = tall // SOURCE_PIECES
    load_src = lambda n: pltpu.make_async_copy(
        src.at[quarter * n : quarter * (n + 1), :], sbuf.at[quarter * n : quarter * (n + 1), :], src_sem.at[n]
    )
    group = lambda j: pl.ds(pl.multiple_of(wide * j, wide), wide)
    load_cos = lambda j: pltpu.make_async_copy(cos.at[:, group(j), :], ctab.at[:, group(j), :], cos_sem.at[j])
    loads = [
        pltpu.make_async_copy(a, b, in_sem.at[n])
        for n, (a, b) in enumerate(
            [(phi.at[kind], ptab), (edge.at[kind], etab), (lam, ltab), (lam_t.at[me], lttab), (modes, mtab)]
        )
    ]
    for n in range(SOURCE_PIECES):
        load_src(n).start()
    load_cos(0).start()
    for load in loads:
        load.start()
    for z in range(slab):
        wbuf[g, z : z + 1, :] = jnp.full((1, 128), width[z], jnp.float32)

    barrier = pltpu.get_barrier_semaphore()
    pl.semaphore_signal(barrier, inc=1, device_id=across, device_id_type=MESH)
    for n in range(targets):
        pl.semaphore_signal(barrier, inc=1, device_id=at(lax.rem(me + n, targets)), device_id_type=MESH)
    widths = lambda n, who: remote(wbuf.at[who], wbuf.at[who], w_send.at[n - 1], w_recv.at[who], {"gz": lax.rem(g + n, 4)})

    for n in range(SOURCE_PIECES):
        load_src(n).wait()
        if n == SOURCE_PIECES - 1:
            for j in range(1, pairs):
                load_cos(j).start()
        r = slice(quarter * n, quarter * (n + 1))
        s16[0, r, :], s16[1, r, :] = halves(sbuf[r, :])

    swap = lambda j: remote(xb.at[2 * j + 1 - c], rx.at[j], d_send.at[j], d_recv.at[j], twin)
    swap_a = lambda j: remote(amine.at[j], apeer.at[j], a_send.at[j], a_recv.at[j], across)
    swap_u = lambda j, who: remote(uo.at[j], xo.at[2 * j + who], u_send.at[j], u_recv.at[j], twin)
    piece = lambda t: pl.ds(pl.multiple_of(part * t, part), part)
    send_x = lambda j, n, t, who: remote(
        et.at[j, piece(t), :], rb.at[j, who], x_send.at[j, n], x_recv.at[j, who], at(t)
    )
    send_y = lambda j, n, t, who: remote(msg.at[j, lax.div(t, 2)], rb2.at[j, who], y_send.at[j, n], y_recv.at[j, who], at(t))
    peer_of = lambda n: lax.rem(me + n, targets)
    zero = jnp.zeros((part, 128), jnp.float32)
    lane = lax.broadcasted_iota(jnp.int32, (part, 128), 1)
    total = 4 * slab
    tiles = mtab.shape[1] // 128

    def cell(zz, side):
        zc = zz + side * (depth - 1 - 2 * zz)
        z = depth * side + zc
        row = pl.ds(z, 1)
        return zc, z, cf[side, row, :], cf[1 - side, row, :], cf[2, row, :]

    def coefficients():
        for n in range(1, 4):
            widths(n, lax.rem(g + n, 4)).wait_recv()
        w = wbuf[...].reshape(total, 128)
        z = lax.broadcasted_iota(jnp.int32, (total, 128), 0)
        cf[0] = 2.0 / (w + jnp.where(z == 0, 0.0, pltpu.roll(w, 1, 0)))
        cf[1] = 2.0 / (w + jnp.where(z == total - 1, 0.0, pltpu.roll(w, total - 1, 0)))
        cf[2] = w
        for load in loads:
            load.wait()
        for n in range(2):
            bc[n] = jnp.broadcast_to(etab[:, n : n + 1], (rows, 128))
        for n in range(half + 2):
            mb[n] = jnp.broadcast_to(mtab[n : n + 1, :], (8, mtab.shape[1]))
        eb[lanes:, :] = jnp.zeros((128 - lanes, 128), jnp.float32)

    def transform(which, a, b):
        hi, lo = halves(jnp.concatenate([a, b], axis=1))
        both = lax.dot_general(
            ptab[which], jnp.concatenate([hi, lo], axis=0), NN, preferred_element_type=jnp.float32
        )
        both = both[:rows] + both[rows:]
        return both[:, :128], both[:, 128:]

    def factor(j):
        eigen = bc[0] + ltab[pl.ds(2 * j + c, 1), :]
        ratios = [jnp.zeros((rows, 128), jnp.float32)] * 2
        for zz in range(depth):
            for n, (side, keep) in enumerate([(h, ratio), (1 - h, ratio2)]):
                zc, _z, outer, inner, w = cell(zz, side)
                inverse = 1.0 / ((outer + inner) + w * eigen - outer * ratios[n])
                ratios[n] = inner * inverse
                keep[j, zc] = ratios[n]
                if n == 0:
                    inv[j, zc] = inverse
        ends2[j] = inverse
        cmine[j], cpeer[j] = ratios
        join[j] = 1.0 / (1.0 - ratios[0] * ratios[1])

    def along_x(j):
        load_cos(j).wait()
        dot = lambda a, b: lax.dot_general(s16[a], ctab[b, group(j), :], NT, preferred_element_type=jnp.float32)
        product = dot(0, 0) + dot(1, 0) + dot(0, 1)
        xb[2 * j] = product[:, :128]
        xb[2 * j + 1] = product[:, 128:]

    def first(j):
        for n in range(2):
            if n:
                swap(j).wait_recv()
            for zl in range(0, slab, 2):
                a, b = (slice(rows * y, rows * (y + 1)) for y in (zl, zl + 1))
                block = rx.at[j] if n else xb.at[2 * j + c]
                zc = slab * ((1 - c) if n else c) + zl
                z = depth * h + zc
                a, b = transform(0, block[a, :], block[b, :])
                fh[j, zc] = cf[2, pl.ds(z, 1), :] * a
                fh[j, zc + 1] = cf[2, pl.ds(z + 1, 1), :] * b
        for zz in range(depth):
            zc = cell(zz, h)[0]
            value = fh[j, zc] + ratio[j, before] * value if zz else fh[j, zc]
            vv[j, zc] = value
            before = zc
        value = value * inv[j, before]
        amine[j] = value
        swap_a(j).start()

    def first_back(j):
        x = amine[j] * join[j]
        y = cpeer[j] * x
        for zz in reversed(range(depth)):
            zc, z = cell(zz, h)[:2]
            yc, yz = cell(zz, 1 - h)[:2]
            if zz < depth - 1:
                x = vv[j, zc] * inv[j, zc] + ratio[j, zc] * x
                y = ratio2[j, yc] * y
            for at_z, plane in ((z, x), (yz, y)):
                weighted = bc[1] * plane
                for n in range(2):
                    rows_n = weighted[rows // 2 * n : rows // 2 * (n + 1)]
                    eb[pl.ds(2 * depth * n + at_z, 1), :] = jnp.sum(rows_n, axis=0, keepdims=True)
        et[j] = jnp.transpose(eb[...])[:, :lanes]
        for n in range(targets):
            send_x(j, n, peer_of(n), me).start()

    def cut_factors():
        eigen_k = [
            jnp.broadcast_to(jnp.sum(jnp.where(lane == 2 * j + 1 - c, lttab[...], 0.0), axis=1, keepdims=True), (part, 128))
            for j in range(pairs)
        ]

        def cut_factor(z, ratio):
            row = pl.ds(z, 1)
            lower, upper, w = cf[0, row, :], cf[1, row, :], cf[2, row, :]
            after = []
            for j in range(pairs):
                for q in range(tiles):
                    col = slice(128 * q, 128 * q + 128)
                    inverse = 1.0 / ((lower + upper) + w * (eigen_k[j] + mb[0, :, col]) - lower * ratio[j * tiles + q])
                    ginv[j, z, :, col] = inverse
                    after.append(upper * inverse)
                    gratio[j, z, :, col] = after[-1]
            return tuple(after)

        lax.fori_loop(0, total, cut_factor, (zero,) * (pairs * tiles))

    ahead = 1
    for j in range(ahead):
        along_x(j)
    pl.semaphore_wait(barrier, targets + 1)
    for n in range(1, 4):
        widths(n, g).start()
    for j in range(ahead):
        swap(j).start()

    def start_x(j, carry):
        along_x(j)
        swap(j).start()
        return carry

    lax.fori_loop(ahead, pairs, start_x, 0)
    coefficients()

    def blocks(j, carry):
        factor(j)
        first(j)
        first_back(j)
        return carry

    lax.fori_loop(0, pairs, blocks, 0)
    cut_factors()

    terms = lambda q: range(half) if q < tiles // 2 else range(half, cuts)
    mode = lambda m: 1 + (m if m < half else m - half)

    def cut(j, carry):
        for n in range(targets):
            t = peer_of(n)
            send_x(j, n, t, t).wait_recv()
        edge = [rb[j, 2 * i] + rb[j, 2 * i + 1] for i in range(parts)]
        even, odd = ([e[:, k : k + 2 * depth] for e in edge] for k in (0, 2 * depth))
        jump = [(even[i] - even[i + 1]) - (odd[i] + odd[i + 1]) for i in range(cuts)]
        mixed = [jump[i] - jump[cuts - 1 - i] for i in range(half)]
        mixed += [jump[i] + jump[cuts - 1 - i] for i in range(half)] + [jump[half]]
        for i in range(cuts):
            gt[i, :, : 2 * depth] = jump[i]
        value = [zero] * tiles
        for z in range(total):
            w = cf[2, z : z + 1, :]
            force = [w * jnp.broadcast_to(m[:, z : z + 1], (part, 128)) for m in mixed]
            for q in range(tiles):
                col = slice(128 * q, 128 * q + 128)
                rhs = gratio[j, z - 1, :, col] * value[q] if z else zero
                for m in terms(q):
                    rhs = rhs + force[m] * mb[mode(m), :, col]
                value[q] = rhs
                gv[z, :, col] = rhs

        x = [zero] * tiles
        sums = [zero] * cuts
        for z in reversed(range(total)):
            along = [zero] * cuts
            for q in range(tiles):
                col = slice(128 * q, 128 * q + 128)
                x[q] = gv[z, :, col] * ginv[j, z, :, col] + gratio[j, z, :, col] * x[q]
                for m in terms(q):
                    along[m] = along[m] + mb[mode(m), :, col] * x[q]
            for m in range(cuts):
                sums[m] = jnp.where(lane == z, jnp.sum(along[m], axis=1, keepdims=True), sums[m])
        true = [zero] * cuts
        for i in range(half):
            true[i] = gt[i] - (sums[half + i] + sums[i])
            true[cuts - 1 - i] = gt[cuts - 1 - i] - (sums[half + i] - sums[i])
        true[half] = gt[half] - sums[cuts - 1]
        for q in range(parts):
            left = true[q - 1] if q else zero
            right = true[q] if q < parts - 1 else zero
            msg[j, q] = ((left - right) + pltpu.roll(left + right, 2 * depth, 1))[:, :lanes]
        for n in range(targets):
            send_y(j, n, peer_of(n), me).start()
        return carry

    gt[...] = jnp.zeros(gt.shape, jnp.float32)
    lax.fori_loop(0, pairs, cut, 0)

    def second(j):
        for n in range(targets):
            t = peer_of(n)
            send_y(j, n, t, t).wait_recv()
        e2[...] = jnp.transpose(rb2[j].reshape(128, lanes))
        def pull(z, w):
            mode_rows = [slice(rows // 2 * n, rows // 2 * (n + 1)) for n in range(2)]
            return jnp.concatenate([bc[1, r] * (w * e2[pl.ds(2 * depth * n + z, 1), :]) for n, r in enumerate(mode_rows)])

        for zz in range(depth):
            zc, z, _outer, _inner, w = cell(zz, h)
            force = fh[j, zc] + pull(z, w)
            value = force + ratio[j, before] * value if zz else force
            vv[j, zc] = value
            before = zc
            zc, z, _outer, _inner, w = cell(zz, 1 - h)
            force = pull(z, w)
            other = force + ratio2[j, before2] * other if zz else force
            before2 = zc
        swap_a(j).wait_recv()
        x = (value * inv[j, before] + cmine[j] * (apeer[j] + other * ends2[j])) * join[j]
        for zz in reversed(range(depth)):
            zc = cell(zz, h)[0]
            if zz < depth - 1:
                x = vv[j, zc] * inv[j, zc] + ratio[j, zc] * x
            fh[j, zc] = x
        for n in range(2):
            for zl in range(0, slab, 2):
                a, b = (slice(rows * y, rows * (y + 1)) for y in (zl, zl + 1))
                zc = slab * (c if n else (1 - c)) + zl
                block = xo.at[2 * j + c] if n else uo.at[j]
                block[a, :], block[b, :] = transform(1, fh[j, zc], fh[j, zc + 1])
            if n == 0:
                swap_u(j, c).start()

    def back_x(j):
        swap_u(j, 1 - c).wait_recv()
        for n in range(2):
            s16[0, :, 128 * n : 128 * n + 128], s16[1, :, 128 * n : 128 * n + 128] = halves(xo[2 * j + n])
        for n in range(pairs):
            i = slice(wide * n, wide * (n + 1))
            dot = lambda a, b: lax.dot_general(
                s16[a, :, :wide], ctab[b, group(j), i], NN, preferred_element_type=jnp.float32
            )
            out[:, i] = out[:, i] + (dot(0, 0) + dot(1, 0) + dot(0, 1))

    def tail(step, carry):
        @pl.when(step < pairs)
        def _():
            second(step)

        @pl.when(step >= 1)
        def _():
            back_x(step - 1)

        return carry

    out[...] = jnp.zeros(out.shape, jnp.float32)
    lax.fori_loop(0, pairs + 1, tail, 0)

    for n in range(1, 4):
        widths(n, g).wait_send()
    for j in range(pairs):
        for n in range(targets):
            send_x(j, n, peer_of(n), me).wait_send()
            send_y(j, n, peer_of(n), me).wait_send()
        swap(j).wait_send()
        swap_a(j).wait_send()
        swap_u(j, c).wait_send()


def fused(source, cell_width):
    slab, rows, nx = source.shape
    parts = lax.axis_size("pa")
    pairs, depth, targets = nx // 256, 2 * slab, 2 * parts
    part = 128 // targets
    ny = rows * parts
    consts = tables(nx, ny, parts, depth)
    f32, b16, V = jnp.float32, jnp.bfloat16, pltpu.VMEM
    tall = slab * rows
    lines = (pairs, depth, rows, 128)
    plane = (pairs, rows, 128)
    sem = lambda *n: pltpu.SemaphoreType.DMA(n)
    lanes = 4 * depth
    small = (pairs, targets, part, lanes)
    scratch = [
        V((tall, nx), f32), V((2, tall, nx), b16), V((2, nx, nx), b16), V((2, 2 * rows, 2 * rows), b16), V((rows, 128), f32),
        V(consts[3].shape, f32), V((part, 128), f32), V(consts[5].shape, f32), V((4, slab, 128), f32),
        V((3, 4 * slab, 128), f32), V((2, rows, 128), f32),
        V((2 * pairs, tall, 128), f32), V((pairs, tall, 128), f32), V(lines, f32), V(lines, f32), V(lines, f32), V(lines, f32),
        V(lines, f32), V(plane, f32), V(plane, f32), V(plane, f32), V(plane, f32), V(plane, f32), V(plane, f32),
        V((128, 128), f32), V((pairs, 128, lanes), f32), V(small, f32), V((parts, part, 128), f32),
        V((parts // 2 + 1, 8, ny), f32), V((pairs, 2 * depth, part, ny), f32), V((pairs, 2 * depth, part, ny), f32), V((2 * depth, part, ny), f32),
        V((pairs, parts, part, lanes), f32), V(small, f32), V((lanes, 128), f32),
        V((pairs, tall, 128), f32), V((2 * pairs, tall, 128), f32),
        sem(5), sem(SOURCE_PIECES), sem(pairs), sem(3), sem(4), sem(pairs), sem(pairs),
        sem(pairs), sem(pairs), sem(pairs, targets), sem(pairs, targets), sem(pairs, targets), sem(pairs, targets),
        sem(pairs), sem(pairs),
    ]
    hbm = pl.BlockSpec(memory_space=pltpu.HBM)
    out = pl.pallas_call(
        functools.partial(fused_kernel, (parts, slab, rows, depth, pairs, part)),
        out_shape=pltpu.VMEM((tall, nx), f32),
        in_specs=[hbm, pl.BlockSpec(memory_space=pltpu.SMEM)] + [hbm] * 6,
        out_specs=pl.BlockSpec(memory_space=pltpu.VMEM),
        scratch_shapes=scratch,
        compiler_params=pltpu.CompilerParams(
            collective_id=0, has_side_effects=True, vmem_limit_bytes=60 * 1024 * 1024
        ),
    )(source.reshape(tall, nx), cell_width, *(jnp.asarray(t) for t in consts))
    return out.reshape(slab, rows, nx)


def fits(source, parts, blocks):
    slab, rows, nx = source.shape
    return (
        blocks == 4 and parts == 8 and nx % 256 == 0 and slab == 8 and rows % 16 == 0
        and (rows * parts) % 256 == 0
    )


def per_device(source, cell_width):
    if fits(source, lax.axis_size("pa"), lax.axis_size("gz")):
        return fused(source, cell_width)
    return on_device(source, cell_width)


def solution(mesh):
    in_specs = (P("gz", "pa", None), P("gz"))
    out_specs = P("gz", "pa", None)
    return jax.shard_map(
        per_device, mesh=mesh, in_specs=in_specs, out_specs=out_specs, check_vma=False
    )
```

```python
import functools

import jax
import jax.numpy as jnp
import numpy as np
from jax import lax
from jax.experimental import pallas as pl
from jax.experimental.pallas import tpu as pltpu
from jax.sharding import PartitionSpec as P

HIGH = lax.Precision.HIGH


def summed_angles(width, coarse, fine, sine):
    f32 = lambda x: jnp.asarray(x.astype(np.float32))
    ca, sa = f32(np.cos(coarse))[:, None, :], f32(np.sin(coarse))[:, None, :]
    cb, sb = f32(np.cos(fine))[None, :, :], f32(np.sin(fine))[None, :, :]
    table = sa * cb + ca * sb if sine else ca * cb - sa * sb
    return table.reshape(width, width)


def split_steps(width):
    step = next(b for b in (32, 16, 8, 1) if width % b == 0)
    return np.arange(0, width, step, dtype=np.int64)[:, None], np.arange(step, dtype=np.int64)[:, None]


def cosine_table(width):
    odd = 2 * np.arange(width, dtype=np.int64)[None, :] + 1
    a, b = (k * odd % (4 * width) * (np.pi / (2 * width)) for k in split_steps(width))
    first = jnp.arange(width)[:, None] == 0
    weights = jnp.where(first, np.sqrt(1.0 / width), np.sqrt(2.0 / width)).astype(jnp.float32)
    return weights * summed_angles(width, a, b, False)


def sine_table(width):
    j = np.arange(1, width + 1, dtype=np.int64)[None, :]
    coarse, fine = split_steps(width)
    a, b = (l * j % (2 * (width + 1)) * (np.pi / (width + 1)) for l in (coarse, fine + 1))
    return np.float32(np.sqrt(2.0 / (width + 1))) * summed_angles(width, a, b, True)


def eigen_first(offset, count, width):
    values = 4.0 * np.sin(np.arange(width) * (np.pi / (2 * width))) ** 2
    return lax.dynamic_slice_in_dim(jnp.asarray(values, jnp.float32), offset, count)[:, None]


def eigen_second(width):
    values = 4.0 * np.sin(np.arange(1, width + 1) * (np.pi / (2 * (width + 1)))) ** 2
    return jnp.asarray(values, jnp.float32)[None, :]


def tiles(rows, width, body):
    lanes = 256 if width % 256 == 0 else width

    if rows % 8:
        for c in range(0, width, lanes):
            body(slice(0, rows), pl.ds(c, lanes))
        return

    def step(r, carry):
        row = pl.ds(pl.multiple_of(r * 8, 8), 8)
        for c in range(0, width, lanes):
            body(row, pl.ds(c, lanes))
        return carry

    lax.fori_loop(0, rows // 8, step, 0)


def ends_kernel(coef, ex, ey, spectral, ends):
    depth, rows, width = spectral.shape

    def body(row, col):
        eigen = ex[row, :] + ey[:, col]
        diag = [coef[0, z] + coef[1, z] + coef[2, z] * eigen for z in range(depth)]
        force = [coef[2, z] * spectral[z, row, col] for z in range(depth)]
        inverse = 1.0 / diag[0]
        value = force[0] * inverse
        other = 1.0 / diag[depth - 1]
        front = force[depth - 1] * other
        for z in range(1, depth):
            inverse = 1.0 / (diag[z] - (coef[0, z] * coef[1, z - 1]) * inverse)
            value = (force[z] + coef[0, z] * value) * inverse
            y = depth - 1 - z
            other = 1.0 / (diag[y] - (coef[1, y] * coef[0, y + 1]) * other)
            front = (force[y] + coef[1, y] * front) * other
        ends[0, row, col] = front
        ends[1, row, col] = value

    tiles(rows, width, body)


def reduced_kernel(coef, ex, ey, ends, sides):
    blocks = ends.shape[0] // 2
    rows, width = ends.shape[1:]
    depth = coef.shape[1] // blocks

    def body(row, col):
        eigen = ex[row, :] + ey[:, col]
        p = jnp.zeros_like(eigen)
        q = jnp.zeros_like(eigen)
        saved = []
        for b in range(blocks):
            s = b * depth
            diag = [coef[0, s + z] + coef[1, s + z] + coef[2, s + z] * eigen for z in range(depth)]
            inverse = 1.0 / diag[0]
            v1 = coef[0, s] * inverse
            other = 1.0 / diag[depth - 1]
            w0 = coef[1, s + depth - 1] * other
            for z in range(1, depth):
                inverse = 1.0 / (diag[z] - (coef[0, s + z] * coef[1, s + z - 1]) * inverse)
                v1 = v1 * (coef[0, s + z] * inverse)
                y = depth - 1 - z
                other = 1.0 / (diag[y] - (coef[1, s + y] * coef[0, s + y + 1]) * other)
                w0 = w0 * (coef[1, s + y] * other)
            w1 = coef[1, s + depth - 1] * inverse
            v0 = coef[0, s] * other
            scale = 1.0 / (1.0 - v0 * q)
            a = (ends[2 * b, row, col] + v0 * p) * scale
            c = w0 * scale
            p, q = ends[2 * b + 1, row, col] + v1 * (p + q * a), v1 * q * c + w1
            saved.append((a, c, p, q))
        head = jnp.zeros_like(eigen)
        for b in reversed(range(blocks)):
            a, c, p, q = saved[b]
            sides[2 * b + 1, row, col] = head
            if b + 1 < blocks:
                sides[2 * b + 2, row, col] = p + q * head
            head = a + c * head
        sides[0, row, col] = jnp.zeros_like(eigen)

    tiles(rows, width, body)


def final_kernel(coef, ex, ey, spectral, sides, solved):
    depth, rows, width = spectral.shape

    def body(row, col):
        eigen = ex[row, :] + ey[:, col]
        ratios, values = [], []
        for z in range(depth):
            diag = coef[0, z] + coef[1, z] + coef[2, z] * eigen
            force = coef[2, z] * spectral[z, row, col]
            if z == 0:
                force = force + coef[0, z] * sides[0, row, col]
            else:
                diag = diag - coef[0, z] * ratios[-1]
                force = force + coef[0, z] * values[-1]
            if z == depth - 1:
                force = force + coef[1, z] * sides[1, row, col]
            inverse = 1.0 / diag
            ratios.append(coef[1, z] * inverse)
            values.append(force * inverse)
        x = values[-1]
        solved[depth - 1, row, col] = x
        for z in reversed(range(depth - 1)):
            x = values[z] + ratios[z] * x
            solved[z, row, col] = x

    tiles(rows, width, body)


def solve_call(kernel, leads, lead_out, coef, ex, ey, *planes):
    rows, width = planes[0].shape[1:]
    block = next((b for b in (32, 24, 16, 8) if rows % b == 0), rows)
    spec = lambda lead: pl.BlockSpec((lead, block, width), lambda i: (0, i, 0))
    return pl.pallas_call(
        kernel,
        grid=(rows // block,),
        in_specs=[
            pl.BlockSpec(memory_space=pltpu.SMEM),
            pl.BlockSpec((block, 1), lambda i: (i, 0)),
            pl.BlockSpec((1, width), lambda i: (0, 0)),
        ]
        + [spec(lead) for lead in leads],
        out_specs=spec(lead_out),
        out_shape=jax.ShapeDtypeStruct((lead_out, rows, width), jnp.float32),
    )(coef, ex, ey, *planes)


def on_device(source, cell_width):
    depth, rows_local, width_x = source.shape
    blocks = lax.axis_size("gz")
    width_y = rows_local * lax.axis_size("pa")
    cos_table = cosine_table(width_x)
    sin_table = sine_table(width_y)
    block = lax.axis_index("gz")
    widths = lax.all_gather(cell_width, "gz", tiled=True)
    padded = jnp.pad(widths, 1)
    coef = jnp.stack(
        [2.0 / (padded[:-2] + widths), 2.0 / (widths + padded[2:]), widths]
    )
    own = lax.dynamic_slice_in_dim(coef, block * depth, depth, axis=1)
    along_x = jnp.einsum("zyi,ki->zky", source, cos_table, precision=HIGH)
    spectral = jnp.einsum(
        "zkj,lj->zkl",
        lax.all_to_all(along_x, "pa", split_axis=1, concat_axis=2, tiled=True),
        sin_table,
        precision=HIGH,
    )
    kx = spectral.shape[1]
    first = lax.axis_index("pa") * kx
    part = kx // blocks
    ex = eigen_first(first, kx, width_x)
    ex_part = eigen_first(first + block * part, part, width_x)
    ey = eigen_second(width_y)
    ends = solve_call(ends_kernel, (depth,), 2, own, ex, ey, spectral)
    ends = lax.all_to_all(ends, "gz", split_axis=1, concat_axis=0, tiled=True)
    sides = solve_call(reduced_kernel, (2 * blocks,), 2 * blocks, coef, ex_part, ey, ends)
    sides = lax.all_to_all(sides, "gz", split_axis=0, concat_axis=1, tiled=True)
    solved = solve_call(final_kernel, (depth, 2), depth, own, ex, ey, spectral, sides)
    along_y = jnp.einsum("zkl,lj->zkj", solved, sin_table, precision=HIGH)
    return jnp.einsum(
        "zky,ki->zyi",
        lax.all_to_all(along_y, "pa", split_axis=2, concat_axis=1, tiled=True),
        cos_table,
        precision=HIGH,
    )


MESH = pl.DeviceIdType.MESH
NT = (((1,), (1,)), ((), ()))
NN = (((1,), (0,)), ((), ()))
SOURCE_PIECES = 4


def halves(x):
    hi = x.astype(jnp.bfloat16)
    return hi, (x - hi.astype(jnp.float32)).astype(jnp.bfloat16)


def block_modes(rows, kind):
    j, l = np.arange(rows), np.arange(rows)[:, None]
    if kind == 1:
        scale = np.sqrt(np.where(l == 0, 1.0, 2.0) / rows)
        angle = np.pi * l / rows
        vectors = scale * np.cos(angle * (2 * j + 1) / 2)
    else:
        angle = (2 * l + 1) * np.pi / (2 * rows + 1)
        vectors = 2.0 / np.sqrt(2 * rows + 1) * np.sin(angle * (j + 1))
    order = np.concatenate([j[::2], j[1::2]])
    vectors, values = vectors[order], 4.0 * np.sin(angle[order, 0] / 2) ** 2
    if kind == 2:
        vectors = vectors[:, ::-1]
    edge = vectors[:, 0] if kind else vectors[:, -1] * np.where(np.arange(rows) < rows // 2, 1.0, -1.0)
    return vectors, values, edge


def stacked(table):
    hi = table.astype(jnp.bfloat16)
    lo = (table - np.asarray(hi, np.float64)).astype(jnp.bfloat16)
    return np.block([[hi, hi], [lo, np.zeros_like(lo)]])


def tables(width, height, parts, depth):
    k, i = np.arange(width)[:, None], np.arange(width)[None, :]
    cos = np.sqrt(np.where(k == 0, 1.0, 2.0) / width) * np.cos(np.pi * (k * (2 * i + 1) % (4 * width)) / (2 * width))
    cos_hi = cos.astype(jnp.bfloat16)
    cos_lo = (cos - np.asarray(cos_hi, np.float64)).astype(jnp.bfloat16)
    rows = height // parts
    phi, edge = [], np.zeros((3, rows, 128), np.float32)
    for kind in range(3):
        vectors, values, ends = block_modes(rows, kind)
        phi.append(np.stack([stacked(vectors), stacked(vectors.T)]))
        edge[kind, :, 0], edge[kind, :, 1] = values, ends
    lam = (4.0 * np.sin(np.arange(width) * np.pi / (2 * width)) ** 2).astype(np.float32).reshape(-1, 128)
    groups = lam.shape[0]
    targets = 2 * parts
    lam_t = np.zeros((targets, 128 // targets, 128), np.float32)
    lam_t[:, :, :groups] = lam.T.reshape(targets, 128 // targets, groups)
    lam = np.pad(lam, ((0, -groups % 8), (0, 0)))
    l = np.arange(1, height + 1)
    l = np.concatenate([l[::2], l[1::2]])[None, :]
    cut = (np.arange(1, parts // 2 + 1) * rows)[:, None]
    sine = lambda j: np.sqrt(2.0 / (height + 1)) * np.sin(np.pi * (l * j % (2 * (height + 1))) / (height + 1))
    modes = np.concatenate([4.0 * np.sin(np.pi * l / (2 * (height + 1))) ** 2, sine(cut) - sine(cut + 1)])
    modes = np.pad(modes, ((0, -len(modes) % 8), (0, 0))).astype(np.float32)
    return np.stack([cos_hi, cos_lo]), np.stack(phi), edge, lam, lam_t, modes


def fused_kernel(
    size, src, width, cos, phi, edge, lam, lam_t, modes, out,
    sbuf, s16, ctab, ptab, etab, ltab, lttab, mtab, wbuf, cf, bc, xb, rx, fh, inv, vv, ratio,
    ratio2, cmine, cpeer, join, ends2, amine, apeer, eb, et, rb, gt, mb, ginv, gratio, gv, msg, rb2, e2, uo, xo,
    in_sem, src_sem, cos_sem, w_send, w_recv, d_send, d_recv, a_send, a_recv,
    x_send, x_recv, y_send, y_recv, u_send, u_recv,
):
    parts, slab, rows, depth, pairs, part = size
    targets = 2 * parts
    wide, lanes = 256, 4 * depth
    tall = slab * rows
    cuts, half = parts - 1, (parts - 1) // 2
    p, g = lax.axis_index("pa"), lax.axis_index("gz")
    h, c = lax.div(g, 2), lax.rem(g, 2)
    me = 2 * p + h
    kind = jnp.where(p == 0, 0, jnp.where(p == parts - 1, 2, 1))
    twin = {"gz": 2 * h + 1 - c}
    across = {"gz": 2 * (1 - h) + c}
    at = lambda t: {"pa": lax.div(t, 2), "gz": 2 * lax.rem(t, 2) + 1 - c}

    def remote(source, target, send, recv, device):
        return pltpu.make_async_remote_copy(
            src_ref=source, dst_ref=target, send_sem=send, recv_sem=recv, device_id=device, device_id_type=MESH
        )

    quarter = tall // SOURCE_PIECES
    load_src = lambda n: pltpu.make_async_copy(
        src.at[quarter * n : quarter * (n + 1), :], sbuf.at[quarter * n : quarter * (n + 1), :], src_sem.at[n]
    )
    group = lambda j: pl.ds(pl.multiple_of(wide * j, wide), wide)
    load_cos = lambda j: pltpu.make_async_copy(cos.at[:, group(j), :], ctab.at[:, group(j), :], cos_sem.at[j])
    loads = [
        pltpu.make_async_copy(a, b, in_sem.at[n])
        for n, (a, b) in enumerate(
            [(phi.at[kind], ptab), (edge.at[kind], etab), (lam, ltab), (lam_t.at[me], lttab), (modes, mtab)]
        )
    ]
    for load in loads:
        load.start()
    for n in range(SOURCE_PIECES):
        load_src(n).start()
    load_cos(0).start()
    for z in range(slab):
        wbuf[g, z : z + 1, :] = jnp.full((1, 128), width[z], jnp.float32)

    barrier = pltpu.get_barrier_semaphore()
    pl.semaphore_signal(barrier, inc=1, device_id=across, device_id_type=MESH)
    for n in range(targets):
        pl.semaphore_signal(barrier, inc=1, device_id=at(lax.rem(me + n, targets)), device_id_type=MESH)
    widths = lambda n, who: remote(wbuf.at[who], wbuf.at[who], w_send.at[n - 1], w_recv.at[who], {"gz": lax.rem(g + n, 4)})

    out[...] = jnp.zeros(out.shape, jnp.float32)
    gt[...] = jnp.zeros(gt.shape, jnp.float32)
    for load in loads:
        load.wait()
    for n in range(2):
        bc[n] = jnp.broadcast_to(etab[:, n : n + 1], (rows, 128))
    for n in range(half + 2):
        mb[n] = jnp.broadcast_to(mtab[n : n + 1, :], (8, mtab.shape[1]))
    eb[lanes:, :] = jnp.zeros((128 - lanes, 128), jnp.float32)

    for n in range(SOURCE_PIECES):
        load_src(n).wait()
        if n == SOURCE_PIECES - 1:
            for j in range(1, pairs):
                load_cos(j).start()
        r = slice(quarter * n, quarter * (n + 1))
        s16[0, r, :], s16[1, r, :] = halves(sbuf[r, :])

    swap = lambda j: remote(xb.at[2 * j + 1 - c], rx.at[j], d_send.at[j], d_recv.at[j], twin)
    swap_a = lambda j: remote(amine.at[j], apeer.at[j], a_send.at[j], a_recv.at[j], across)
    swap_u = lambda j, who: remote(uo.at[j], xo.at[2 * j + who], u_send.at[j], u_recv.at[j], twin)
    piece = lambda t: pl.ds(pl.multiple_of(part * t, part), part)
    send_x = lambda j, n, t, who: remote(
        et.at[j, piece(t), :], rb.at[j, who], x_send.at[j, n], x_recv.at[j, who], at(t)
    )
    send_y = lambda j, n, t, who: remote(msg.at[j, lax.div(t, 2)], rb2.at[j, who], y_send.at[j, n], y_recv.at[j, who], at(t))
    peer_of = lambda n: lax.rem(me + n, targets)
    zero = jnp.zeros((part, 128), jnp.float32)
    lane = lax.broadcasted_iota(jnp.int32, (part, 128), 1)
    total = 4 * slab
    tiles = mtab.shape[1] // 128

    def cell(zz, side):
        zc = zz + side * (depth - 1 - 2 * zz)
        z = depth * side + zc
        row = pl.ds(z, 1)
        return zc, z, cf[side, row, :], cf[1 - side, row, :], cf[2, row, :]

    def coefficients():
        for n in range(1, 4):
            widths(n, lax.rem(g + n, 4)).wait_recv()
        w = wbuf[...].reshape(total, 128)
        z = lax.broadcasted_iota(jnp.int32, (total, 128), 0)
        cf[0] = 2.0 / (w + jnp.where(z == 0, 0.0, pltpu.roll(w, 1, 0)))
        cf[1] = 2.0 / (w + jnp.where(z == total - 1, 0.0, pltpu.roll(w, total - 1, 0)))
        cf[2] = w

    def transform(which, a, b):
        hi, lo = halves(jnp.concatenate([a, b], axis=1))
        both = lax.dot_general(
            ptab[which], jnp.concatenate([hi, lo], axis=0), NN, preferred_element_type=jnp.float32
        )
        both = both[:rows] + both[rows:]
        return both[:, :128], both[:, 128:]

    def factor(j):
        eigen = bc[0] + ltab[pl.ds(2 * j + c, 1), :]
        ratios = [jnp.zeros((rows, 128), jnp.float32)] * 2
        for zz in range(depth):
            for n, (side, keep) in enumerate([(h, ratio), (1 - h, ratio2)]):
                zc, _z, outer, inner, w = cell(zz, side)
                inverse = 1.0 / ((outer + inner) + w * eigen - outer * ratios[n])
                ratios[n] = inner * inverse
                keep[j, zc] = ratios[n]
                if n == 0:
                    inv[j, zc] = inverse
        ends2[j] = inverse
        cmine[j], cpeer[j] = ratios
        join[j] = 1.0 / (1.0 - ratios[0] * ratios[1])

    def along_x(j):
        load_cos(j).wait()
        table = [ctab[n, group(j), :] for n in range(2)]
        product = lax.dot_general(
            jnp.concatenate([s16[0], s16[1], s16[0]], axis=1), jnp.concatenate([table[0], table[0], table[1]], axis=1),
            NT, preferred_element_type=jnp.float32,
        )
        xb[2 * j] = product[:, :128]
        xb[2 * j + 1] = product[:, 128:]

    def first(j):
        for n in range(2):
            if n:
                swap(j).wait_recv()
            for zl in range(0, slab, 2):
                a, b = (slice(rows * y, rows * (y + 1)) for y in (zl, zl + 1))
                block = rx.at[j] if n else xb.at[2 * j + c]
                zc = slab * ((1 - c) if n else c) + zl
                z = depth * h + zc
                a, b = transform(0, block[a, :], block[b, :])
                fh[j, zc] = cf[2, pl.ds(z, 1), :] * a
                fh[j, zc + 1] = cf[2, pl.ds(z + 1, 1), :] * b
        for zz in range(depth):
            zc = cell(zz, h)[0]
            value = fh[j, zc] + ratio[j, before] * value if zz else fh[j, zc]
            vv[j, zc] = value
            before = zc
        value = value * inv[j, before]
        amine[j] = value
        swap_a(j).start()

    def first_back(j):
        x = amine[j] * join[j]
        y = cpeer[j] * x
        for zz in reversed(range(depth)):
            zc, z = cell(zz, h)[:2]
            yc, yz = cell(zz, 1 - h)[:2]
            if zz < depth - 1:
                x = vv[j, zc] * inv[j, zc] + ratio[j, zc] * x
                y = ratio2[j, yc] * y
            for at_z, plane in ((z, x), (yz, y)):
                weighted = bc[1] * plane
                for n in range(2):
                    rows_n = weighted[rows // 2 * n : rows // 2 * (n + 1)]
                    eb[pl.ds(2 * depth * n + at_z, 1), :] = jnp.sum(rows_n, axis=0, keepdims=True)
        et[j] = jnp.transpose(eb[...])[:, :lanes]
        for n in range(targets):
            send_x(j, n, peer_of(n), me).start()

    def cut_factors():
        eigen_k = [
            jnp.broadcast_to(jnp.sum(jnp.where(lane == 2 * j + 1 - c, lttab[...], 0.0), axis=1, keepdims=True), (part, 128))
            for j in range(pairs)
        ]

        def cut_factor(z, ratio):
            row = pl.ds(z, 1)
            lower, upper, w = cf[0, row, :], cf[1, row, :], cf[2, row, :]
            after = []
            for j in range(pairs):
                for q in range(tiles):
                    col = slice(128 * q, 128 * q + 128)
                    inverse = 1.0 / ((lower + upper) + w * (eigen_k[j] + mb[0, :, col]) - lower * ratio[j * tiles + q])
                    ginv[j, z, :, col] = inverse
                    after.append(upper * inverse)
                    gratio[j, z, :, col] = after[-1]
            return tuple(after)

        lax.fori_loop(0, total, cut_factor, (zero,) * (pairs * tiles))

    ahead = 1
    for j in range(ahead):
        along_x(j)
    pl.semaphore_wait(barrier, targets + 1)
    for n in range(1, 4):
        widths(n, g).start()
    for j in range(ahead):
        swap(j).start()

    def start_x(j, carry):
        along_x(j)
        swap(j).start()
        return carry

    lax.fori_loop(ahead, pairs, start_x, 0)
    coefficients()

    def blocks(j, carry):
        factor(j)
        first(j)
        first_back(j)
        return carry

    lax.fori_loop(0, pairs, blocks, 0)
    cut_factors()

    terms = lambda q: range(half) if q < tiles // 2 else range(half, cuts)
    mode = lambda m: 1 + (m if m < half else m - half)

    def cut(j, carry):
        for n in range(targets):
            t = peer_of(n)
            send_x(j, n, t, t).wait_recv()
        edge = [rb[j, 2 * i] + rb[j, 2 * i + 1] for i in range(parts)]
        even, odd = ([e[:, k : k + 2 * depth] for e in edge] for k in (0, 2 * depth))
        jump = [(even[i] - even[i + 1]) - (odd[i] + odd[i + 1]) for i in range(cuts)]
        mixed = [jump[i] - jump[cuts - 1 - i] for i in range(half)]
        mixed += [jump[i] + jump[cuts - 1 - i] for i in range(half)] + [jump[half]]
        for i in range(cuts):
            gt[i, :, : 2 * depth] = jump[i]
        value = [zero] * tiles
        for z in range(total):
            w = cf[2, z : z + 1, :]
            force = [w * jnp.broadcast_to(m[:, z : z + 1], (part, 128)) for m in mixed]
            for q in range(tiles):
                col = slice(128 * q, 128 * q + 128)
                rhs = gratio[j, z - 1, :, col] * value[q] if z else zero
                for m in terms(q):
                    rhs = rhs + force[m] * mb[mode(m), :, col]
                value[q] = rhs
                gv[z, :, col] = rhs

        x = [zero] * tiles
        sums = [zero] * cuts
        for z in reversed(range(total)):
            along = [zero] * cuts
            for q in range(tiles):
                col = slice(128 * q, 128 * q + 128)
                x[q] = gv[z, :, col] * ginv[j, z, :, col] + gratio[j, z, :, col] * x[q]
                for m in terms(q):
                    along[m] = along[m] + mb[mode(m), :, col] * x[q]
            for m in range(cuts):
                sums[m] = jnp.where(lane == z, jnp.sum(along[m], axis=1, keepdims=True), sums[m])
        true = [zero] * cuts
        for i in range(half):
            true[i] = gt[i] - (sums[half + i] + sums[i])
            true[cuts - 1 - i] = gt[cuts - 1 - i] - (sums[half + i] - sums[i])
        true[half] = gt[half] - sums[cuts - 1]
        for q in range(parts):
            left = true[q - 1] if q else zero
            right = true[q] if q < parts - 1 else zero
            msg[j, q] = ((left - right) + pltpu.roll(left + right, 2 * depth, 1))[:, :lanes]
        for n in range(targets):
            send_y(j, n, peer_of(n), me).start()
        return carry

    lax.fori_loop(0, pairs, cut, 0)

    def second(j):
        for n in range(targets):
            t = peer_of(n)
            send_y(j, n, t, t).wait_recv()
        e2[...] = jnp.transpose(rb2[j].reshape(128, lanes))
        def pull(z, w):
            mode_rows = [slice(rows // 2 * n, rows // 2 * (n + 1)) for n in range(2)]
            return jnp.concatenate([bc[1, r] * (w * e2[pl.ds(2 * depth * n + z, 1), :]) for n, r in enumerate(mode_rows)])

        for zz in range(depth):
            zc, z, _outer, _inner, w = cell(zz, h)
            force = fh[j, zc] + pull(z, w)
            value = force + ratio[j, before] * value if zz else force
            vv[j, zc] = value
            before = zc
            zc, z, _outer, _inner, w = cell(zz, 1 - h)
            force = pull(z, w)
            other = force + ratio2[j, before2] * other if zz else force
            before2 = zc
        swap_a(j).wait_recv()
        x = (value * inv[j, before] + cmine[j] * (apeer[j] + other * ends2[j])) * join[j]
        for zz in reversed(range(depth)):
            zc = cell(zz, h)[0]
            if zz < depth - 1:
                x = vv[j, zc] * inv[j, zc] + ratio[j, zc] * x
            fh[j, zc] = x
        for n in range(2):
            for zl in range(0, slab, 2):
                a, b = (slice(rows * y, rows * (y + 1)) for y in (zl, zl + 1))
                zc = slab * (c if n else (1 - c)) + zl
                block = xo.at[2 * j + c] if n else uo.at[j]
                block[a, :], block[b, :] = transform(1, fh[j, zc], fh[j, zc + 1])
            if n == 0:
                swap_u(j, c).start()

    def back_x(j):
        swap_u(j, 1 - c).wait_recv()
        for n in range(2):
            s16[0, :, 128 * n : 128 * n + 128], s16[1, :, 128 * n : 128 * n + 128] = halves(xo[2 * j + n])
        for n in range(pairs):
            i = slice(wide * n, wide * (n + 1))
            hi, lo = s16[0, :, :wide], s16[1, :, :wide]
            table = [ctab[m, group(j), i] for m in range(2)]
            out[:, i] = out[:, i] + lax.dot_general(
                jnp.concatenate([hi, lo, hi], axis=1), jnp.concatenate([table[0], table[0], table[1]], axis=0),
                NN, preferred_element_type=jnp.float32,
            )

    def tail(step, carry):
        @pl.when(step < pairs)
        def _():
            second(step)

        @pl.when(step >= 1)
        def _():
            back_x(step - 1)

        return carry

    lax.fori_loop(0, pairs + 1, tail, 0)

    for n in range(1, 4):
        widths(n, g).wait_send()
    for j in range(pairs):
        for n in range(targets):
            send_x(j, n, peer_of(n), me).wait_send()
            send_y(j, n, peer_of(n), me).wait_send()
        swap(j).wait_send()
        swap_a(j).wait_send()
        swap_u(j, c).wait_send()


def fused(source, cell_width):
    slab, rows, nx = source.shape
    parts = lax.axis_size("pa")
    pairs, depth, targets = nx // 256, 2 * slab, 2 * parts
    part = 128 // targets
    ny = rows * parts
    consts = tables(nx, ny, parts, depth)
    f32, b16, V = jnp.float32, jnp.bfloat16, pltpu.VMEM
    tall = slab * rows
    lines = (pairs, depth, rows, 128)
    plane = (pairs, rows, 128)
    sem = lambda *n: pltpu.SemaphoreType.DMA(n)
    lanes = 4 * depth
    small = (pairs, targets, part, lanes)
    scratch = [
        V((tall, nx), f32), V((2, tall, nx), b16), V((2, nx, nx), b16), V((2, 2 * rows, 2 * rows), b16), V((rows, 128), f32),
        V(consts[3].shape, f32), V((part, 128), f32), V(consts[5].shape, f32), V((4, slab, 128), f32),
        V((3, 4 * slab, 128), f32), V((2, rows, 128), f32),
        V((2 * pairs, tall, 128), f32), V((pairs, tall, 128), f32), V(lines, f32), V(lines, f32), V(lines, f32), V(lines, f32),
        V(lines, f32), V(plane, f32), V(plane, f32), V(plane, f32), V(plane, f32), V(plane, f32), V(plane, f32),
        V((128, 128), f32), V((pairs, 128, lanes), f32), V(small, f32), V((parts, part, 128), f32),
        V((parts // 2 + 1, 8, ny), f32), V((pairs, 2 * depth, part, ny), f32), V((pairs, 2 * depth, part, ny), f32), V((2 * depth, part, ny), f32),
        V((pairs, parts, part, lanes), f32), V(small, f32), V((lanes, 128), f32),
        V((pairs, tall, 128), f32), V((2 * pairs, tall, 128), f32),
        sem(5), sem(SOURCE_PIECES), sem(pairs), sem(3), sem(4), sem(pairs), sem(pairs),
        sem(pairs), sem(pairs), sem(pairs, targets), sem(pairs, targets), sem(pairs, targets), sem(pairs, targets),
        sem(pairs), sem(pairs),
    ]
    hbm = pl.BlockSpec(memory_space=pltpu.HBM)
    out = pl.pallas_call(
        functools.partial(fused_kernel, (parts, slab, rows, depth, pairs, part)),
        out_shape=pltpu.VMEM((tall, nx), f32),
        in_specs=[hbm, pl.BlockSpec(memory_space=pltpu.SMEM)] + [hbm] * 6,
        out_specs=pl.BlockSpec(memory_space=pltpu.VMEM),
        scratch_shapes=scratch,
        compiler_params=pltpu.CompilerParams(
            collective_id=0, has_side_effects=True, vmem_limit_bytes=60 * 1024 * 1024
        ),
    )(source.reshape(tall, nx), cell_width, *(jnp.asarray(t) for t in consts))
    return out.reshape(slab, rows, nx)


def fits(source, parts, blocks):
    slab, rows, nx = source.shape
    return (
        blocks == 4 and parts == 8 and nx % 256 == 0 and slab == 8 and rows % 16 == 0
        and (rows * parts) % 256 == 0
    )


def per_device(source, cell_width):
    if fits(source, lax.axis_size("pa"), lax.axis_size("gz")):
        return fused(source, cell_width)
    return on_device(source, cell_width)


def solution(mesh):
    in_specs = (P("gz", "pa", None), P("gz"))
    out_specs = P("gz", "pa", None)
    return jax.shard_map(
        per_device, mesh=mesh, in_specs=in_specs, out_specs=out_specs, check_vma=False
    )
```

```python
import functools

import jax
import jax.numpy as jnp
import numpy as np
from jax import lax
from jax.experimental import pallas as pl
from jax.experimental.pallas import tpu as pltpu
from jax.sharding import PartitionSpec as P

HIGH = lax.Precision.HIGH


def summed_angles(width, coarse, fine, sine):
    f32 = lambda x: jnp.asarray(x.astype(np.float32))
    ca, sa = f32(np.cos(coarse))[:, None, :], f32(np.sin(coarse))[:, None, :]
    cb, sb = f32(np.cos(fine))[None, :, :], f32(np.sin(fine))[None, :, :]
    table = sa * cb + ca * sb if sine else ca * cb - sa * sb
    return table.reshape(width, width)


def split_steps(width):
    step = next(b for b in (32, 16, 8, 1) if width % b == 0)
    return np.arange(0, width, step, dtype=np.int64)[:, None], np.arange(step, dtype=np.int64)[:, None]


def cosine_table(width):
    odd = 2 * np.arange(width, dtype=np.int64)[None, :] + 1
    a, b = (k * odd % (4 * width) * (np.pi / (2 * width)) for k in split_steps(width))
    first = jnp.arange(width)[:, None] == 0
    weights = jnp.where(first, np.sqrt(1.0 / width), np.sqrt(2.0 / width)).astype(jnp.float32)
    return weights * summed_angles(width, a, b, False)


def sine_table(width):
    j = np.arange(1, width + 1, dtype=np.int64)[None, :]
    coarse, fine = split_steps(width)
    a, b = (l * j % (2 * (width + 1)) * (np.pi / (width + 1)) for l in (coarse, fine + 1))
    return np.float32(np.sqrt(2.0 / (width + 1))) * summed_angles(width, a, b, True)


def eigen_first(offset, count, width):
    values = 4.0 * np.sin(np.arange(width) * (np.pi / (2 * width))) ** 2
    return lax.dynamic_slice_in_dim(jnp.asarray(values, jnp.float32), offset, count)[:, None]


def eigen_second(width):
    values = 4.0 * np.sin(np.arange(1, width + 1) * (np.pi / (2 * (width + 1)))) ** 2
    return jnp.asarray(values, jnp.float32)[None, :]


def tiles(rows, width, body):
    lanes = 256 if width % 256 == 0 else width

    if rows % 8:
        for c in range(0, width, lanes):
            body(slice(0, rows), pl.ds(c, lanes))
        return

    def step(r, carry):
        row = pl.ds(pl.multiple_of(r * 8, 8), 8)
        for c in range(0, width, lanes):
            body(row, pl.ds(c, lanes))
        return carry

    lax.fori_loop(0, rows // 8, step, 0)


def ends_kernel(coef, ex, ey, spectral, ends):
    depth, rows, width = spectral.shape

    def body(row, col):
        eigen = ex[row, :] + ey[:, col]
        diag = [coef[0, z] + coef[1, z] + coef[2, z] * eigen for z in range(depth)]
        force = [coef[2, z] * spectral[z, row, col] for z in range(depth)]
        inverse = 1.0 / diag[0]
        value = force[0] * inverse
        other = 1.0 / diag[depth - 1]
        front = force[depth - 1] * other
        for z in range(1, depth):
            inverse = 1.0 / (diag[z] - (coef[0, z] * coef[1, z - 1]) * inverse)
            value = (force[z] + coef[0, z] * value) * inverse
            y = depth - 1 - z
            other = 1.0 / (diag[y] - (coef[1, y] * coef[0, y + 1]) * other)
            front = (force[y] + coef[1, y] * front) * other
        ends[0, row, col] = front
        ends[1, row, col] = value

    tiles(rows, width, body)


def reduced_kernel(coef, ex, ey, ends, sides):
    blocks = ends.shape[0] // 2
    rows, width = ends.shape[1:]
    depth = coef.shape[1] // blocks

    def body(row, col):
        eigen = ex[row, :] + ey[:, col]
        p = jnp.zeros_like(eigen)
        q = jnp.zeros_like(eigen)
        saved = []
        for b in range(blocks):
            s = b * depth
            diag = [coef[0, s + z] + coef[1, s + z] + coef[2, s + z] * eigen for z in range(depth)]
            inverse = 1.0 / diag[0]
            v1 = coef[0, s] * inverse
            other = 1.0 / diag[depth - 1]
            w0 = coef[1, s + depth - 1] * other
            for z in range(1, depth):
                inverse = 1.0 / (diag[z] - (coef[0, s + z] * coef[1, s + z - 1]) * inverse)
                v1 = v1 * (coef[0, s + z] * inverse)
                y = depth - 1 - z
                other = 1.0 / (diag[y] - (coef[1, s + y] * coef[0, s + y + 1]) * other)
                w0 = w0 * (coef[1, s + y] * other)
            w1 = coef[1, s + depth - 1] * inverse
            v0 = coef[0, s] * other
            scale = 1.0 / (1.0 - v0 * q)
            a = (ends[2 * b, row, col] + v0 * p) * scale
            c = w0 * scale
            p, q = ends[2 * b + 1, row, col] + v1 * (p + q * a), v1 * q * c + w1
            saved.append((a, c, p, q))
        head = jnp.zeros_like(eigen)
        for b in reversed(range(blocks)):
            a, c, p, q = saved[b]
            sides[2 * b + 1, row, col] = head
            if b + 1 < blocks:
                sides[2 * b + 2, row, col] = p + q * head
            head = a + c * head
        sides[0, row, col] = jnp.zeros_like(eigen)

    tiles(rows, width, body)


def final_kernel(coef, ex, ey, spectral, sides, solved):
    depth, rows, width = spectral.shape

    def body(row, col):
        eigen = ex[row, :] + ey[:, col]
        ratios, values = [], []
        for z in range(depth):
            diag = coef[0, z] + coef[1, z] + coef[2, z] * eigen
            force = coef[2, z] * spectral[z, row, col]
            if z == 0:
                force = force + coef[0, z] * sides[0, row, col]
            else:
                diag = diag - coef[0, z] * ratios[-1]
                force = force + coef[0, z] * values[-1]
            if z == depth - 1:
                force = force + coef[1, z] * sides[1, row, col]
            inverse = 1.0 / diag
            ratios.append(coef[1, z] * inverse)
            values.append(force * inverse)
        x = values[-1]
        solved[depth - 1, row, col] = x
        for z in reversed(range(depth - 1)):
            x = values[z] + ratios[z] * x
            solved[z, row, col] = x

    tiles(rows, width, body)


def solve_call(kernel, leads, lead_out, coef, ex, ey, *planes):
    rows, width = planes[0].shape[1:]
    block = next((b for b in (32, 24, 16, 8) if rows % b == 0), rows)
    spec = lambda lead: pl.BlockSpec((lead, block, width), lambda i: (0, i, 0))
    return pl.pallas_call(
        kernel,
        grid=(rows // block,),
        in_specs=[
            pl.BlockSpec(memory_space=pltpu.SMEM),
            pl.BlockSpec((block, 1), lambda i: (i, 0)),
            pl.BlockSpec((1, width), lambda i: (0, 0)),
        ]
        + [spec(lead) for lead in leads],
        out_specs=spec(lead_out),
        out_shape=jax.ShapeDtypeStruct((lead_out, rows, width), jnp.float32),
    )(coef, ex, ey, *planes)


def on_device(source, cell_width):
    depth, rows_local, width_x = source.shape
    blocks = lax.axis_size("gz")
    width_y = rows_local * lax.axis_size("pa")
    cos_table = cosine_table(width_x)
    sin_table = sine_table(width_y)
    block = lax.axis_index("gz")
    widths = lax.all_gather(cell_width, "gz", tiled=True)
    padded = jnp.pad(widths, 1)
    coef = jnp.stack(
        [2.0 / (padded[:-2] + widths), 2.0 / (widths + padded[2:]), widths]
    )
    own = lax.dynamic_slice_in_dim(coef, block * depth, depth, axis=1)
    along_x = jnp.einsum("zyi,ki->zky", source, cos_table, precision=HIGH)
    spectral = jnp.einsum(
        "zkj,lj->zkl",
        lax.all_to_all(along_x, "pa", split_axis=1, concat_axis=2, tiled=True),
        sin_table,
        precision=HIGH,
    )
    kx = spectral.shape[1]
    first = lax.axis_index("pa") * kx
    part = kx // blocks
    ex = eigen_first(first, kx, width_x)
    ex_part = eigen_first(first + block * part, part, width_x)
    ey = eigen_second(width_y)
    ends = solve_call(ends_kernel, (depth,), 2, own, ex, ey, spectral)
    ends = lax.all_to_all(ends, "gz", split_axis=1, concat_axis=0, tiled=True)
    sides = solve_call(reduced_kernel, (2 * blocks,), 2 * blocks, coef, ex_part, ey, ends)
    sides = lax.all_to_all(sides, "gz", split_axis=0, concat_axis=1, tiled=True)
    solved = solve_call(final_kernel, (depth, 2), depth, own, ex, ey, spectral, sides)
    along_y = jnp.einsum("zkl,lj->zkj", solved, sin_table, precision=HIGH)
    return jnp.einsum(
        "zky,ki->zyi",
        lax.all_to_all(along_y, "pa", split_axis=2, concat_axis=1, tiled=True),
        cos_table,
        precision=HIGH,
    )


MESH = pl.DeviceIdType.MESH
NT = (((1,), (1,)), ((), ()))
NN = (((1,), (0,)), ((), ()))
SOURCE_PIECES = 4


def halves(x):
    hi = x.astype(jnp.bfloat16)
    return hi, (x - hi.astype(jnp.float32)).astype(jnp.bfloat16)


def block_modes(rows, kind):
    j, l = np.arange(rows), np.arange(rows)[:, None]
    if kind == 1:
        scale = np.sqrt(np.where(l == 0, 1.0, 2.0) / rows)
        angle = np.pi * l / rows
        vectors = scale * np.cos(angle * (2 * j + 1) / 2)
    else:
        angle = (2 * l + 1) * np.pi / (2 * rows + 1)
        vectors = 2.0 / np.sqrt(2 * rows + 1) * np.sin(angle * (j + 1))
    order = np.concatenate([j[::2], j[1::2]])
    vectors, values = vectors[order], 4.0 * np.sin(angle[order, 0] / 2) ** 2
    if kind == 2:
        vectors = vectors[:, ::-1]
    edge = vectors[:, 0] if kind else vectors[:, -1] * np.where(np.arange(rows) < rows // 2, 1.0, -1.0)
    return vectors, values, edge


def stacked(table):
    hi = table.astype(jnp.bfloat16)
    lo = (table - np.asarray(hi, np.float64)).astype(jnp.bfloat16)
    return np.block([[hi, hi], [lo, np.zeros_like(lo)]])


def tables(width, height, parts, depth):
    k, i = np.arange(width)[:, None], np.arange(width)[None, :]
    cos = np.sqrt(np.where(k == 0, 1.0, 2.0) / width) * np.cos(np.pi * (k * (2 * i + 1) % (4 * width)) / (2 * width))
    cos_hi = cos.astype(jnp.bfloat16)
    cos_lo = (cos - np.asarray(cos_hi, np.float64)).astype(jnp.bfloat16)
    rows = height // parts
    phi, edge = [], np.zeros((3, rows, 128), np.float32)
    for kind in range(3):
        vectors, values, ends = block_modes(rows, kind)
        phi.append(np.stack([stacked(vectors), stacked(vectors.T)]))
        edge[kind, :, 0], edge[kind, :, 1] = values, ends
    lam = (4.0 * np.sin(np.arange(width) * np.pi / (2 * width)) ** 2).astype(np.float32).reshape(-1, 128)
    groups = lam.shape[0]
    targets = 2 * parts
    lam_t = np.zeros((targets, 128 // targets, 128), np.float32)
    lam_t[:, :, :groups] = lam.T.reshape(targets, 128 // targets, groups)
    lam = np.pad(lam, ((0, -groups % 8), (0, 0)))
    l = np.arange(1, height + 1)
    l = np.concatenate([l[::2], l[1::2]])[None, :]
    cut = (np.arange(1, parts // 2 + 1) * rows)[:, None]
    sine = lambda j: np.sqrt(2.0 / (height + 1)) * np.sin(np.pi * (l * j % (2 * (height + 1))) / (height + 1))
    modes = np.concatenate([4.0 * np.sin(np.pi * l / (2 * (height + 1))) ** 2, sine(cut) - sine(cut + 1)])
    modes = np.pad(modes, ((0, -len(modes) % 8), (0, 0))).astype(np.float32)
    return np.stack([cos_hi, cos_lo]), np.stack(phi), edge, lam, lam_t, modes


def fused_kernel(
    size, src, width, cos, phi, edge, lam, lam_t, modes, out,
    sbuf, s16, ctab, ptab, etab, ltab, lttab, mtab, wbuf, cf, bc, xb, rx, fh, inv, vv, ratio,
    ratio2, cmine, cpeer, join, ends2, amine, apeer, eb, et, rb, gt, mb, ginv, gratio, gv, msg, rb2, e2, uo, xo,
    in_sem, src_sem, cos_sem, w_send, w_recv, d_send, d_recv, a_send, a_recv,
    x_send, x_recv, y_send, y_recv, u_send, u_recv,
):
    parts, slab, rows, depth, pairs, part = size
    targets = 2 * parts
    wide, lanes = 256, 4 * depth
    tall = slab * rows
    cuts, half = parts - 1, (parts - 1) // 2
    p, g = lax.axis_index("pa"), lax.axis_index("gz")
    h, c = lax.div(g, 2), lax.rem(g, 2)
    me = 2 * p + h
    kind = jnp.where(p == 0, 0, jnp.where(p == parts - 1, 2, 1))
    twin = {"gz": 2 * h + 1 - c}
    across = {"gz": 2 * (1 - h) + c}
    at = lambda t: {"pa": lax.div(t, 2), "gz": 2 * lax.rem(t, 2) + 1 - c}

    def remote(source, target, send, recv, device):
        return pltpu.make_async_remote_copy(
            src_ref=source, dst_ref=target, send_sem=send, recv_sem=recv, device_id=device, device_id_type=MESH
        )

    quarter = tall // SOURCE_PIECES
    load_src = lambda n: pltpu.make_async_copy(
        src.at[quarter * n : quarter * (n + 1), :], sbuf.at[quarter * n : quarter * (n + 1), :], src_sem.at[n]
    )
    group = lambda j: pl.ds(pl.multiple_of(wide * j, wide), wide)
    load_cos = lambda j: pltpu.make_async_copy(cos.at[:, group(j), :], ctab.at[:, group(j), :], cos_sem.at[j])
    loads = [
        pltpu.make_async_copy(a, b, in_sem.at[n])
        for n, (a, b) in enumerate(
            [(phi.at[kind], ptab), (edge.at[kind], etab), (lam, ltab), (lam_t.at[me], lttab), (modes, mtab)]
        )
    ]
    for load in loads:
        load.start()
    for n in range(SOURCE_PIECES):
        load_src(n).start()
    load_cos(0).start()
    for z in range(slab):
        wbuf[g, z : z + 1, :] = jnp.full((1, 128), width[z], jnp.float32)

    barrier = pltpu.get_barrier_semaphore()
    pl.semaphore_signal(barrier, inc=1, device_id=across, device_id_type=MESH)
    for n in range(targets):
        pl.semaphore_signal(barrier, inc=1, device_id=at(lax.rem(me + n, targets)), device_id_type=MESH)
    widths = lambda n, who: remote(wbuf.at[who], wbuf.at[who], w_send.at[n - 1], w_recv.at[who], {"gz": lax.rem(g + n, 4)})

    out[...] = jnp.zeros(out.shape, jnp.float32)
    gt[...] = jnp.zeros(gt.shape, jnp.float32)
    for load in loads:
        load.wait()
    for n in range(2):
        bc[n] = jnp.broadcast_to(etab[:, n : n + 1], (rows, 128))
    for n in range(half + 2):
        mb[n] = jnp.broadcast_to(mtab[n : n + 1, :], (8, mtab.shape[1]))
    eb[lanes:, :] = jnp.zeros((128 - lanes, 128), jnp.float32)

    for n in range(SOURCE_PIECES):
        load_src(n).wait()
        if n == SOURCE_PIECES - 1:
            for j in range(1, pairs):
                load_cos(j).start()
        r = slice(quarter * n, quarter * (n + 1))
        s16[0, r, :], s16[1, r, :] = halves(sbuf[r, :])

    swap = lambda j: remote(xb.at[2 * j + 1 - c], rx.at[j], d_send.at[j], d_recv.at[j], twin)
    swap_a = lambda j: remote(amine.at[j], apeer.at[j], a_send.at[j], a_recv.at[j], across)
    swap_u = lambda j, who: remote(uo.at[j], xo.at[2 * j + who], u_send.at[j], u_recv.at[j], twin)
    piece = lambda t: pl.ds(pl.multiple_of(part * t, part), part)
    send_x = lambda j, n, t, who: remote(
        et.at[j, piece(t), :], rb.at[j, who], x_send.at[j, n], x_recv.at[j, who], at(t)
    )
    send_y = lambda j, n, t, who: remote(msg.at[j, lax.div(t, 2)], rb2.at[j, who], y_send.at[j, n], y_recv.at[j, who], at(t))
    upper_half = lax.div(me, parts)
    peer_of = lambda n: upper_half * n + (1 - upper_half) * (targets - 1 - n)
    zero = jnp.zeros((part, 128), jnp.float32)
    lane = lax.broadcasted_iota(jnp.int32, (part, 128), 1)
    total = 4 * slab
    tiles = mtab.shape[1] // 128

    def cell(zz, side):
        zc = zz + side * (depth - 1 - 2 * zz)
        z = depth * side + zc
        row = pl.ds(z, 1)
        return zc, z, cf[side, row, :], cf[1 - side, row, :], cf[2, row, :]

    def coefficients():
        for n in range(1, 4):
            widths(n, lax.rem(g + n, 4)).wait_recv()
        w = wbuf[...].reshape(total, 128)
        z = lax.broadcasted_iota(jnp.int32, (total, 128), 0)
        cf[0] = 2.0 / (w + jnp.where(z == 0, 0.0, pltpu.roll(w, 1, 0)))
        cf[1] = 2.0 / (w + jnp.where(z == total - 1, 0.0, pltpu.roll(w, total - 1, 0)))
        cf[2] = w

    def transform(which, a, b):
        hi, lo = halves(jnp.concatenate([a, b], axis=1))
        both = lax.dot_general(
            ptab[which], jnp.concatenate([hi, lo], axis=0), NN, preferred_element_type=jnp.float32
        )
        both = both[:rows] + both[rows:]
        return both[:, :128], both[:, 128:]

    def factor(j):
        eigen = bc[0] + ltab[pl.ds(2 * j + c, 1), :]
        ratios = [jnp.zeros((rows, 128), jnp.float32)] * 2
        for zz in range(depth):
            for n, (side, keep) in enumerate([(h, ratio), (1 - h, ratio2)]):
                zc, _z, outer, inner, w = cell(zz, side)
                inverse = 1.0 / ((outer + inner) + w * eigen - outer * ratios[n])
                ratios[n] = inner * inverse
                keep[j, zc] = ratios[n]
                if n == 0:
                    inv[j, zc] = inverse
        ends2[j] = inverse
        cmine[j], cpeer[j] = ratios
        join[j] = 1.0 / (1.0 - ratios[0] * ratios[1])

    def along_x(j):
        load_cos(j).wait()
        table = [ctab[n, group(j), :] for n in range(2)]
        product = lax.dot_general(
            jnp.concatenate([s16[0], s16[1], s16[0]], axis=1), jnp.concatenate([table[0], table[0], table[1]], axis=1),
            NT, preferred_element_type=jnp.float32,
        )
        xb[2 * j] = product[:, :128]
        xb[2 * j + 1] = product[:, 128:]

    def first(j):
        for n in range(2):
            if n:
                swap(j).wait_recv()
            for zl in range(0, slab, 2):
                a, b = (slice(rows * y, rows * (y + 1)) for y in (zl, zl + 1))
                block = rx.at[j] if n else xb.at[2 * j + c]
                zc = slab * ((1 - c) if n else c) + zl
                z = depth * h + zc
                a, b = transform(0, block[a, :], block[b, :])
                fh[j, zc] = cf[2, pl.ds(z, 1), :] * a
                fh[j, zc + 1] = cf[2, pl.ds(z + 1, 1), :] * b
        for zz in range(depth):
            zc = cell(zz, h)[0]
            value = fh[j, zc] + ratio[j, before] * value if zz else fh[j, zc]
            vv[j, zc] = value
            before = zc
        value = value * inv[j, before]
        amine[j] = value
        swap_a(j).start()

    def first_back(j):
        x = amine[j] * join[j]
        y = cpeer[j] * x
        for zz in reversed(range(depth)):
            zc, z = cell(zz, h)[:2]
            yc, yz = cell(zz, 1 - h)[:2]
            if zz < depth - 1:
                x = vv[j, zc] * inv[j, zc] + ratio[j, zc] * x
                y = ratio2[j, yc] * y
            for at_z, plane in ((z, x), (yz, y)):
                weighted = bc[1] * plane
                for n in range(2):
                    rows_n = weighted[rows // 2 * n : rows // 2 * (n + 1)]
                    eb[pl.ds(2 * depth * n + at_z, 1), :] = jnp.sum(rows_n, axis=0, keepdims=True)
        et[j] = jnp.transpose(eb[...])[:, :lanes]
        for n in range(targets):
            send_x(j, n, peer_of(n), me).start()

    def cut_factors():
        eigen_k = [
            jnp.broadcast_to(jnp.sum(jnp.where(lane == 2 * j + 1 - c, lttab[...], 0.0), axis=1, keepdims=True), (part, 128))
            for j in range(pairs)
        ]

        def cut_factor(z, ratio):
            row = pl.ds(z, 1)
            lower, upper, w = cf[0, row, :], cf[1, row, :], cf[2, row, :]
            after = []
            for j in range(pairs):
                for q in range(tiles):
                    col = slice(128 * q, 128 * q + 128)
                    inverse = 1.0 / ((lower + upper) + w * (eigen_k[j] + mb[0, :, col]) - lower * ratio[j * tiles + q])
                    ginv[j, z, :, col] = inverse
                    after.append(upper * inverse)
                    gratio[j, z, :, col] = after[-1]
            return tuple(after)

        lax.fori_loop(0, total, cut_factor, (zero,) * (pairs * tiles))

    ahead = 1
    for j in range(ahead):
        along_x(j)
    pl.semaphore_wait(barrier, targets + 1)
    for n in range(1, 4):
        widths(n, g).start()
    for j in range(ahead):
        swap(j).start()

    def start_x(j, carry):
        along_x(j)
        swap(j).start()
        return carry

    lax.fori_loop(ahead, pairs, start_x, 0)
    coefficients()

    def blocks(j, carry):
        factor(j)
        first(j)
        first_back(j)
        return carry

    lax.fori_loop(0, pairs, blocks, 0)
    cut_factors()

    terms = lambda q: range(half) if q < tiles // 2 else range(half, cuts)
    mode = lambda m: 1 + (m if m < half else m - half)

    def cut(j, carry):
        for n in range(targets):
            t = peer_of(n)
            send_x(j, n, t, t).wait_recv()
        edge = [rb[j, 2 * i] + rb[j, 2 * i + 1] for i in range(parts)]
        even, odd = ([e[:, k : k + 2 * depth] for e in edge] for k in (0, 2 * depth))
        jump = [(even[i] - even[i + 1]) - (odd[i] + odd[i + 1]) for i in range(cuts)]
        mixed = [jump[i] - jump[cuts - 1 - i] for i in range(half)]
        mixed += [jump[i] + jump[cuts - 1 - i] for i in range(half)] + [jump[half]]
        for i in range(cuts):
            gt[i, :, : 2 * depth] = jump[i]
        value = [zero] * tiles
        for z in range(total):
            w = cf[2, z : z + 1, :]
            force = [w * jnp.broadcast_to(m[:, z : z + 1], (part, 128)) for m in mixed]
            for q in range(tiles):
                col = slice(128 * q, 128 * q + 128)
                rhs = gratio[j, z - 1, :, col] * value[q] if z else zero
                for m in terms(q):
                    rhs = rhs + force[m] * mb[mode(m), :, col]
                value[q] = rhs
                gv[z, :, col] = rhs

        x = [zero] * tiles
        sums = [zero] * cuts
        for z in reversed(range(total)):
            along = [zero] * cuts
            for q in range(tiles):
                col = slice(128 * q, 128 * q + 128)
                x[q] = gv[z, :, col] * ginv[j, z, :, col] + gratio[j, z, :, col] * x[q]
                for m in terms(q):
                    along[m] = along[m] + mb[mode(m), :, col] * x[q]
            for m in range(cuts):
                sums[m] = jnp.where(lane == z, jnp.sum(along[m], axis=1, keepdims=True), sums[m])
        true = [zero] * cuts
        for i in range(half):
            true[i] = gt[i] - (sums[half + i] + sums[i])
            true[cuts - 1 - i] = gt[cuts - 1 - i] - (sums[half + i] - sums[i])
        true[half] = gt[half] - sums[cuts - 1]
        for q in range(parts):
            left = true[q - 1] if q else zero
            right = true[q] if q < parts - 1 else zero
            msg[j, q] = ((left - right) + pltpu.roll(left + right, 2 * depth, 1))[:, :lanes]
        for n in range(targets):
            send_y(j, n, peer_of(n), me).start()
        return carry

    lax.fori_loop(0, pairs, cut, 0)

    def second(j):
        for n in range(targets):
            t = peer_of(n)
            send_y(j, n, t, t).wait_recv()
        e2[...] = jnp.transpose(rb2[j].reshape(128, lanes))
        def pull(z, w):
            mode_rows = [slice(rows // 2 * n, rows // 2 * (n + 1)) for n in range(2)]
            return jnp.concatenate([bc[1, r] * (w * e2[pl.ds(2 * depth * n + z, 1), :]) for n, r in enumerate(mode_rows)])

        for zz in range(depth):
            zc, z, _outer, _inner, w = cell(zz, h)
            force = fh[j, zc] + pull(z, w)
            value = force + ratio[j, before] * value if zz else force
            vv[j, zc] = value
            before = zc
            zc, z, _outer, _inner, w = cell(zz, 1 - h)
            force = pull(z, w)
            other = force + ratio2[j, before2] * other if zz else force
            before2 = zc
        swap_a(j).wait_recv()
        x = (value * inv[j, before] + cmine[j] * (apeer[j] + other * ends2[j])) * join[j]
        for zz in reversed(range(depth)):
            zc = cell(zz, h)[0]
            if zz < depth - 1:
                x = vv[j, zc] * inv[j, zc] + ratio[j, zc] * x
            fh[j, zc] = x
        for n in range(2):
            for zl in range(0, slab, 2):
                a, b = (slice(rows * y, rows * (y + 1)) for y in (zl, zl + 1))
                zc = slab * (c if n else (1 - c)) + zl
                block = xo.at[2 * j + c] if n else uo.at[j]
                block[a, :], block[b, :] = transform(1, fh[j, zc], fh[j, zc + 1])
            if n == 0:
                swap_u(j, c).start()

    def back_x(j):
        swap_u(j, 1 - c).wait_recv()
        for n in range(2):
            s16[0, :, 128 * n : 128 * n + 128], s16[1, :, 128 * n : 128 * n + 128] = halves(xo[2 * j + n])
        for n in range(pairs):
            i = slice(wide * n, wide * (n + 1))
            hi, lo = s16[0, :, :wide], s16[1, :, :wide]
            table = [ctab[m, group(j), i] for m in range(2)]
            out[:, i] = out[:, i] + lax.dot_general(
                jnp.concatenate([hi, lo, hi], axis=1), jnp.concatenate([table[0], table[0], table[1]], axis=0),
                NN, preferred_element_type=jnp.float32,
            )

    def tail(step, carry):
        @pl.when(step < pairs)
        def _():
            second(step)

        @pl.when(step >= 1)
        def _():
            back_x(step - 1)

        return carry

    lax.fori_loop(0, pairs + 1, tail, 0)

    for n in range(1, 4):
        widths(n, g).wait_send()
    for j in range(pairs):
        for n in range(targets):
            send_x(j, n, peer_of(n), me).wait_send()
            send_y(j, n, peer_of(n), me).wait_send()
        swap(j).wait_send()
        swap_a(j).wait_send()
        swap_u(j, c).wait_send()


def fused(source, cell_width):
    slab, rows, nx = source.shape
    parts = lax.axis_size("pa")
    pairs, depth, targets = nx // 256, 2 * slab, 2 * parts
    part = 128 // targets
    ny = rows * parts
    consts = tables(nx, ny, parts, depth)
    f32, b16, V = jnp.float32, jnp.bfloat16, pltpu.VMEM
    tall = slab * rows
    lines = (pairs, depth, rows, 128)
    plane = (pairs, rows, 128)
    sem = lambda *n: pltpu.SemaphoreType.DMA(n)
    lanes = 4 * depth
    small = (pairs, targets, part, lanes)
    scratch = [
        V((tall, nx), f32), V((2, tall, nx), b16), V((2, nx, nx), b16), V((2, 2 * rows, 2 * rows), b16), V((rows, 128), f32),
        V(consts[3].shape, f32), V((part, 128), f32), V(consts[5].shape, f32), V((4, slab, 128), f32),
        V((3, 4 * slab, 128), f32), V((2, rows, 128), f32),
        V((2 * pairs, tall, 128), f32), V((pairs, tall, 128), f32), V(lines, f32), V(lines, f32), V(lines, f32), V(lines, f32),
        V(lines, f32), V(plane, f32), V(plane, f32), V(plane, f32), V(plane, f32), V(plane, f32), V(plane, f32),
        V((128, 128), f32), V((pairs, 128, lanes), f32), V(small, f32), V((parts, part, 128), f32),
        V((parts // 2 + 1, 8, ny), f32), V((pairs, 2 * depth, part, ny), f32), V((pairs, 2 * depth, part, ny), f32), V((2 * depth, part, ny), f32),
        V((pairs, parts, part, lanes), f32), V(small, f32), V((lanes, 128), f32),
        V((pairs, tall, 128), f32), V((2 * pairs, tall, 128), f32),
        sem(5), sem(SOURCE_PIECES), sem(pairs), sem(3), sem(4), sem(pairs), sem(pairs),
        sem(pairs), sem(pairs), sem(pairs, targets), sem(pairs, targets), sem(pairs, targets), sem(pairs, targets),
        sem(pairs), sem(pairs),
    ]
    hbm = pl.BlockSpec(memory_space=pltpu.HBM)
    out = pl.pallas_call(
        functools.partial(fused_kernel, (parts, slab, rows, depth, pairs, part)),
        out_shape=pltpu.VMEM((tall, nx), f32),
        in_specs=[hbm, pl.BlockSpec(memory_space=pltpu.SMEM)] + [hbm] * 6,
        out_specs=pl.BlockSpec(memory_space=pltpu.VMEM),
        scratch_shapes=scratch,
        compiler_params=pltpu.CompilerParams(
            collective_id=0, has_side_effects=True, vmem_limit_bytes=60 * 1024 * 1024
        ),
    )(source.reshape(tall, nx), cell_width, *(jnp.asarray(t) for t in consts))
    return out.reshape(slab, rows, nx)


def fits(source, parts, blocks):
    slab, rows, nx = source.shape
    return (
        blocks == 4 and parts == 8 and nx % 256 == 0 and slab == 8 and rows % 16 == 0
        and (rows * parts) % 256 == 0
    )


def per_device(source, cell_width):
    if fits(source, lax.axis_size("pa"), lax.axis_size("gz")):
        return fused(source, cell_width)
    return on_device(source, cell_width)


def solution(mesh):
    in_specs = (P("gz", "pa", None), P("gz"))
    out_specs = P("gz", "pa", None)
    return jax.shard_map(
        per_device, mesh=mesh, in_specs=in_specs, out_specs=out_specs, check_vma=False
    )
```
